32 devices in a mesh: task: 4 (over x, core), dp: 8 (over z, y).
Axes of the slice: x: 2, y: 2, z: 4, core: 2. Of those that a mesh axis runs over, the one named last changes fastest.
Arguments:
- inputs: bfloat16 [8192, 4096], P('dp'), may hold values from -6 to 6
- cotangent: bfloat16 [4, 8192, 1024], P('task', 'dp'), may hold values from -0.44194174 to 0.44194174
- task_order: int32 [4], replicated, may hold values from 0 to 3, each once
- conflict_flags: int32 [4, 4], replicated, may hold values 0 or 1
Outputs:
- combined: bfloat16 [4096, 1024], P(None, 'task')
The draws below stay inside these ranges and needn't reach their ends.
Inputs may be any that keep to these rules, and one draw needn't show every extreme that they name: `task_order`: a permutation of the tasks. `conflict_flags`: diagonal entries are ignored.
All inputs are finite; a program needn't handle non-finite values.
Results may differ from the reference program's by a relative error of at most 0.001.
Values may be sent and summed in bfloat16 or wider, within the bound.
A program may use at most 128 MiB of HBM per device.

```python
import math
import jax
import jax.numpy as jnp
from jax import lax

D = 4096
KVW = 1024
TASKS = 4
TOKENS = 8192


def latent_factors(key):
    return jax.random.normal(jax.random.fold_in(key, 21), (TOKENS, 32, 16), jnp.float32)


def draw_inputs(key, part):
    latent = latent_factors(key)
    loading = jax.random.normal(jax.random.fold_in(key, 22), (16, 32, D // 32), jnp.float32) / 4.0
    independent = jax.random.normal(jax.random.fold_in(key, 23), (TOKENS, D), jnp.float32)
    grouped = jnp.einsum('ngr,rgf->ngf', latent, loading).reshape(TOKENS, D)
    values = 0.8 * grouped + 0.6 * independent
    position = jnp.arange(D, dtype=jnp.float32) / (D - 1.0)
    low_end = math.log(0.5)
    high_end = math.log(2.0)
    feature_scale = jnp.exp(low_end + (high_end - low_end) * position)
    values = values * feature_scale[None, :]
    return jnp.clip(values, -6.0, 6.0).astype(jnp.bfloat16)


def draw_cotangent(key, part):
    key_mix = jax.random.fold_in(key, 11)
    key_base = jax.random.fold_in(key, 12)
    key_own = jax.random.fold_in(key, 13)
    key_basis = jax.random.fold_in(key, 15)
    key_signs = jax.random.fold_in(key, 16)
    key_columns = jax.random.fold_in(key, 17)
    key_order = jax.random.fold_in(key, 18)
    key_second = jax.random.fold_in(key, 19)
    key_other = jax.random.fold_in(key, 20)
    sign_values = jnp.where(jax.random.bernoulli(key_order, 0.5, (TASKS,)), 1.0, -1.0).astype(jnp.float32)
    magnitude = jax.random.uniform(key_mix, (TASKS,), jnp.float32, 0.3, 1.0)
    mixing = (sign_values * magnitude)[:, None, None]
    second_mix = jax.random.uniform(key_second, (TASKS, 1, 1), jnp.float32, -1.0, 1.0)
    latent = latent_factors(key)
    basis_rows = jax.random.normal(key_basis, (512, KVW), jnp.float32)
    row_signs = jax.random.uniform(key_signs, (TASKS, 32), jnp.float32, -1.0, 1.0)
    column_scales = jnp.exp(jax.random.uniform(key_columns, (TASKS, 8), jnp.float32, math.log(0.5), math.log(2.0)))
    weighted = (latent[None] * row_signs[:, None, :, None]).reshape(TASKS, TOKENS, 512)
    structured = jnp.einsum('tnk,kc->tnc', weighted, basis_rows)
    structured = structured * jnp.repeat(column_scales, KVW // 8, axis=1)[:, None, :]
    structured = structured * (0.25 / math.sqrt(512.0))
    shared = jnp.clip(jax.random.normal(key_base, (TOKENS, KVW), jnp.float32), -4.0, 4.0)
    other = jnp.clip(jax.random.normal(key_other, (TOKENS, KVW), jnp.float32), -4.0, 4.0)
    private = jnp.clip(jax.random.normal(key_own, (TASKS, TOKENS, KVW), jnp.float32), -4.0, 4.0)
    raw = 0.8 * mixing * shared[None] + second_mix * other[None] + 0.45 * private + structured
    raw = jnp.clip(raw, -4.0, 4.0)
    values = raw / math.sqrt(TOKENS)
    return values.astype(jnp.bfloat16)


def set_ends(values, key, smallest, high):
    index_at = [jax.random.randint(jax.random.fold_in(key, axis), (), 0, length) for axis, length in enumerate(values.shape)]
    main_axis = values.shape.index(max(values.shape))
    beside = index_at[:main_axis] + [(index_at[main_axis] + 1) % values.shape[main_axis]] + index_at[main_axis + 1:]
    return values.at[tuple(index_at)].set(smallest).at[tuple(beside)].set(high)


def setup_inputs(seed: int = 0) -> dict:
    key_of = jax.random.split(jax.random.key(seed), 5)
    inputs = draw_inputs(jax.random.fold_in(key_of[4], 71), 0)
    cotangent = draw_cotangent(jax.random.fold_in(key_of[4], 71), 0)
    task_order = jax.random.permutation(key_of[2], TASKS).astype(jnp.int32)
    conflict_flags = set_ends((jax.random.randint(key_of[3], (TASKS, TASKS), 0, 4) < 3).astype(jnp.int32), jax.random.fold_in(key_of[3], 1), 0, 1)
    return {"inputs": inputs, "cotangent": cotangent, "task_order": task_order, "conflict_flags": conflict_flags}


def project_weights(gram_matrix, task_order, conflict_flags):
    count = gram_matrix.shape[0]
    labels = jnp.arange(count, dtype=jnp.int32)
    coefficients = jnp.eye(count, dtype=jnp.float32)
    for position in range(count):
        target = task_order[position]
        pick_column = (labels == target).astype(jnp.float32)
        column = jnp.dot(gram_matrix, pick_column, precision=lax.Precision.HIGHEST)
        inner_dots = jnp.dot(coefficients, column, precision=lax.Precision.HIGHEST)
        own_square = jnp.sum(pick_column * column)
        active = jnp.dot(conflict_flags.astype(jnp.float32), pick_column, precision=lax.Precision.HIGHEST) * (1.0 - pick_column)
        removed = jnp.minimum(inner_dots, 0.0) / own_square * active
        coefficients = coefficients - removed[:, None] * pick_column[None, :]
    return jnp.sum(coefficients, axis=0)


def reference(inputs, cotangent, task_order, conflict_flags):
    def one_task(task_cot):
        return lax.dot_general(inputs, task_cot, (((0,), (0,)), ((), ())), preferred_element_type=jnp.float32)

    grads = lax.map(one_task, cotangent)
    gram_matrix = jnp.einsum("tab,sab->ts", grads, grads, precision=lax.Precision.HIGHEST)
    weights = project_weights(gram_matrix, task_order, conflict_flags)
    combined = jnp.einsum("t,tab->ab", weights, grads, precision=lax.Precision.HIGHEST)
    return combined.astype(jnp.bfloat16)
```

```python
import functools

import jax
import jax.numpy as jnp
from jax import lax
from jax.experimental import pallas as pl
from jax.experimental.pallas import tpu as pltpu
from jax.sharding import PartitionSpec as P

MESH = pl.DeviceIdType.MESH
TOP = 32767.0
SHARE = (7, 16)


def coded(tile):
    high = jnp.maximum(jnp.max(jnp.abs(tile), axis=0, keepdims=True), 1e-30)
    code = jnp.round(tile * (TOP / high)).astype(jnp.int32).astype(jnp.int16)
    return code, high * (1.0 / TOP)


def decoded(code, scale):
    return code.astype(jnp.int32).astype(jnp.float32) * scale


def plan(tasks, blocks):
    bounds = [j * blocks * SHARE[0] // SHARE[1] for j in range(tasks + 1)]
    return [bounds[j + 1] - bounds[j] for j in range(tasks)]


def kernel(tasks, ndp, blocks, order_ref, flags_ref, x_hbm, c_hbm, out_ref,
           x_ref, xt, cots, ysend_a, yscale_a, yrecv_a, yrscale_a, zsend_a, zscale_a, zrecv_a, zrscale_a, own_a,
           ysend_b, yscale_b, yrecv_b, yrscale_b, zsend_b, zscale_b, zrecv_b, zrscale_b, own_b,
           grads, gram_own, gram_dp, gram_mid, gram_task,
           x_sem, c_sem, cs_sem, cr_sem,
           yas_sem, yar_sem, zas_sem, zar_sem, ybs_sem, ybr_sem, zbs_sem, zbr_sem,
           gs_sem, gr_sem, hs_sem, hr_sem, ns_sem, nr_sem, ms_sem, mr_sem):
    nz = ndp // 2
    far = nz // 2
    pairs_of = tasks // 2
    me_t = lax.axis_index("task")
    me_d = lax.axis_index("dp")
    z = me_d // 2
    y = me_d % 2
    rows = x_ref.shape[1] // ndp
    step = rows // blocks
    width = cots.shape[2]
    first_y = plan(tasks, blocks)
    first_z = [blocks - n for n in first_y]
    base_y = [sum(first_y[:j]) for j in range(tasks)]
    base_z = [sum(first_z[:j]) for j in range(tasks)]

    def zof(k):
        return lax.rem(z + k + nz, nz)

    def dp_at(zi, yi):
        return zi * 2 + yi

    def mate(j, way):
        return (lax.rem(me_t // 2 + way * (j // 2) + pairs_of, pairs_of) * 2 + lax.rem(me_t % 2 + j % 2, 2))

    partner = (me_t, dp_at(z, 1 - y))

    def remote(src, dst, s, r, device):
        return pltpu.make_async_remote_copy(src_ref=src, dst_ref=dst, send_sem=s, recv_sem=r,
                                            device_id=device, device_id_type=MESH)

    x_copies = []
    for d in range(ndp):
        part = pl.ds(d * rows, rows)
        x_copies.append(pltpu.make_async_copy(x_hbm.at[:, part], x_ref.at[:, part], x_sem.at[d]))
    c_copy = pltpu.make_async_copy(c_hbm.at[:, pl.ds(pl.multiple_of(me_t * width, width), width)], cots.at[0], c_sem)
    c_copy.start()
    for copy in x_copies:
        copy.start()

    barrier = pltpu.get_barrier_semaphore()
    for k in range(1, ndp):
        pl.semaphore_signal(barrier, inc=1, device_id=(me_t, lax.rem(me_d + k, ndp)), device_id_type=MESH)
    for k in range(1, tasks):
        pl.semaphore_signal(barrier, inc=1, device_id=(lax.rem(me_t + k, tasks), me_d), device_id_type=MESH)
    pl.semaphore_wait(barrier, ndp + tasks - 2)

    def c_remote(j):
        peer = mate(j, 1)
        return remote(c_hbm.at[:, pl.ds(pl.multiple_of(peer * width, width), width)], cots.at[j],
                      cs_sem.at[j], cr_sem.at[j], (peer, me_d))

    for j in range(1, tasks):
        c_remote(j).start()
    c_copy.wait()
    for copy in x_copies:
        copy.wait()

    def product(j, block, zi, yi):
        index = dp_at(zi, yi) * blocks + block
        if j == 0:
            turned = x_ref[:, pl.ds(pl.multiple_of(index * step, step), step)].T
            xt[index] = turned
        else:
            turned = xt[index]
        return jnp.dot(turned, cots[j], preferred_element_type=jnp.float32)

    def side(u):
        return 1 - 2 * (u % 2)

    def messages(u):
        sign = side(u)
        chain = [(far - h, sign, h, far - h - 1 if h < far else None) for h in range(far, 0, -1)]
        chain += [(nz - 1 - h, -sign, h, nz - 2 - h if h < far - 1 else None) for h in range(far - 1, 0, -1)]
        return chain

    lasts = [far - 1] + ([nz - 2] if nz > 2 else [])

    def ya(u):
        return (remote(ysend_a.at[u], yrecv_a.at[u], yas_sem.at[u, 0], yar_sem.at[u, 0], partner),
                remote(yscale_a.at[u], yrscale_a.at[u], yas_sem.at[u, 1], yar_sem.at[u, 1], partner))

    def yb(u):
        return (remote(ysend_b.at[u], yrecv_b.at[u], ybs_sem.at[u, 0], ybr_sem.at[u, 0], partner),
                remote(yscale_b.at[u], yrscale_b.at[u], ybs_sem.at[u, 1], ybr_sem.at[u, 1], partner))

    def za(u, m, sign):
        peer = (me_t, dp_at(zof(sign), y))
        return (remote(zsend_a.at[u, m], zrecv_a.at[u, m], zas_sem.at[u, m, 0], zar_sem.at[u, m, 0], peer),
                remote(zscale_a.at[u, m], zrscale_a.at[u, m], zas_sem.at[u, m, 1], zar_sem.at[u, m, 1], peer))

    def zb(u, m, sign):
        peer = (me_t, dp_at(zof(sign), y))
        return (remote(zsend_b.at[u, m], zrecv_b.at[u, m], zbs_sem.at[u, m, 0], zbr_sem.at[u, m, 0], peer),
                remote(zscale_b.at[u, m], zrscale_b.at[u, m], zbs_sem.at[u, m, 1], zbr_sem.at[u, m, 1], peer))

    def start(copies):
        for copy in copies:
            copy.start()

    def arrive(copies):
        for copy in copies:
            copy.wait_recv()

    def each(count, body):
        if count:
            lax.fori_loop(0, count, lambda i, carry: (body(i), carry)[1], 0)

    def a_y(j):
        def unit(i):
            u = base_y[j] + i

            def fill(k):
                code, scale = coded(product(j, i, zof(k), 1 - y))
                ysend_a[u, k] = code
                yscale_a[u, k] = scale
            each(nz, fill)
            start(ya(u))
        each(first_y[j], unit)

    def o_y(j):
        def unit(i):
            u = base_y[j] + i

            def fill(k):
                own_a[u, k] = product(j, i, zof(k), y)
            each(nz, fill)
        each(first_y[j], unit)

    def z_part_b(j, i, message):
        u = base_z[j] + i
        m, sign, h, needs = message
        if needs is not None:
            arrive(zb(u, needs, sign))

        def fill(yi):
            total = product(j, first_y[j] + i, zof(sign * h), yi)
            if needs is not None:
                total = total + decoded(zrecv_b[u, needs, yi], zrscale_b[u, needs, yi])
            code, scale = coded(total)
            zsend_b[u, m, yi] = code
            zscale_b[u, m, yi] = scale
        each(2, fill)
        start(zb(u, m, sign))

    def a_z(j):
        each(first_z[j], lambda i: z_part_b(j, i, messages(base_z[j] + i)[0]))

    def b_z(j):
        def unit(i):
            chain = messages(base_z[j] + i)[1:]
            for message in sorted(chain, key=lambda one: one[3] is not None):
                z_part_b(j, i, message)
        each(first_z[j], unit)

    def c_z(j):
        def unit(i):
            u = base_z[j] + i
            arrive(zb(u, lasts[0], side(u)))
            for m in lasts[1:]:
                arrive(zb(u, m, -side(u)))

            def total(yi):
                value = own_b[u, yi]
                for m in lasts:
                    value = value + decoded(zrecv_b[u, m, yi], zrscale_b[u, m, yi])
                return value
            code, scale = coded(total(1 - y))
            ysend_b[u] = code
            yscale_b[u] = scale
            start(yb(u))
            own_b[u, y] = total(y)
        each(first_z[j], unit)

    def o_z(j):
        def unit(i):
            u = base_z[j] + i

            def fill(yi):
                own_b[u, yi] = product(j, first_y[j] + i, z, yi)
            each(2, fill)
        each(first_z[j], unit)

    def task_of(j):
        return mate(j, -1)

    def f_z(j):
        def unit(i):
            u = base_z[j] + i
            arrive(yb(u))
            grads[task_of(j), first_y[j] + i] = own_b[u, y] + decoded(yrecv_b[u], yrscale_b[u])
        each(first_z[j], unit)

    def z_part_a(u, message):
        m, sign, h, needs = message
        k = lax.rem(sign * h + nz, nz)
        total = own_a[u, k] + decoded(yrecv_a[u, k], yrscale_a[u, k])
        if needs is not None:
            arrive(za(u, needs, sign))
            total = total + decoded(zrecv_a[u, needs], zrscale_a[u, needs])
        code, scale = coded(total)
        zsend_a[u, m] = code
        zscale_a[u, m] = scale
        start(za(u, m, sign))

    def b1_y(j):
        def unit(i):
            u = base_y[j] + i
            arrive(ya(u))
            z_part_a(u, messages(u)[0])
        each(first_y[j], unit)

    def b2_y(j):
        def unit(i):
            u = base_y[j] + i
            for message in sorted(messages(u)[1:], key=lambda one: one[3] is not None):
                z_part_a(u, message)
        each(first_y[j], unit)

    def f_y(j):
        def unit(i):
            u = base_y[j] + i
            arrive(za(u, lasts[0], side(u)))
            for m in lasts[1:]:
                arrive(za(u, m, -side(u)))
            total = own_a[u, 0] + decoded(yrecv_a[u, 0], yrscale_a[u, 0])
            for m in lasts:
                total = total + decoded(zrecv_a[u, m], zrscale_a[u, m])
            grads[task_of(j), i] = total
        each(first_y[j], unit)

    for j in range(tasks):
        if j:
            c_remote(j).wait_recv()
        a_z(j)
        a_y(j)
        b_z(j)
        o_z(j)
        o_y(j)
        if j >= 2:
            c_z(j - 2)
            b1_y(j - 2)
    for j in range(max(tasks - 2, 0), tasks):
        b1_y(j)
        c_z(j)
    for j in range(tasks):
        b2_y(j)
    for j in range(tasks):
        f_z(j)
    for j in range(tasks):
        f_y(j)

    pairs = [(s, t) for s in range(tasks) for t in range(s, tasks)]

    def products(index, sums):
        held = [grads[t, index] for t in range(tasks)]
        return tuple(total + jnp.sum((held[s] * held[t]).reshape(step // 8, 8, width), axis=0)
                     for total, (s, t) in zip(sums, pairs))

    sums = lax.fori_loop(0, blocks, products, tuple(jnp.zeros((8, width), jnp.float32) for _ in pairs))
    line = lax.broadcasted_iota(jnp.int32, (8, 128), 0)
    lane = lax.broadcasted_iota(jnp.int32, (8, 128), 1)
    gram = jnp.zeros((8, 128), jnp.float32)
    for total, (s, t) in zip(sums, pairs):
        value = jnp.sum(jnp.sum(total, axis=0, keepdims=True), axis=1, keepdims=True)
        here = ((line == s) & (lane == t)) | ((line == t) & (lane == s))
        gram = gram + jnp.where(here, value, 0.0)

    def swap(value, buffer_own, buffer, count, s_sem, r_sem, device):
        buffer_own[...] = value
        copies = [remote(buffer_own, buffer.at[k], s_sem.at[k], r_sem.at[k], device(k)) for k in range(1, count)]
        start(copies)
        for k, copy in enumerate(copies, 1):
            copy.wait_recv()
            value = value + buffer[k]
        for copy in copies:
            copy.wait_send()
        return value

    gram = swap(gram, gram_own, gram_dp, ndp, gs_sem, gr_sem, lambda k: (me_t, lax.rem(me_d + k, ndp)))
    gram = swap(gram, gram_mid, gram_task, tasks, hs_sem, hr_sem, lambda k: (lax.rem(me_t + k, tasks), me_d))

    cols = [jnp.sum(jnp.where(lane == m, gram, 0.0), axis=1, keepdims=True) for m in range(tasks)]
    entry = lambda column, i: jnp.sum(jnp.where(line[:, :1] == i, column, 0.0), axis=0, keepdims=True)
    row = line[:, :1]
    coefficients = [(row == m).astype(jnp.float32) for m in range(tasks)]
    flag_cols = []
    for m in range(tasks):
        column = jnp.zeros((8, 1), jnp.float32)
        for i in range(tasks):
            column = column + jnp.where(row == i, flags_ref[i, m].astype(jnp.float32), 0.0)
        flag_cols.append(column)
    for position in range(tasks):
        target = order_ref[position]
        picks = [jnp.where(target == m, 1.0, 0.0) for m in range(tasks)]
        column = sum(cols[m] * picks[m] for m in range(tasks))
        dots = sum(coefficients[m] * entry(column, m) for m in range(tasks))
        square = sum(entry(column, m) * picks[m] for m in range(tasks))
        active = sum(flag_cols[m] * picks[m] for m in range(tasks)) * jnp.where(row == target, 0.0, 1.0)
        removed = jnp.minimum(dots, 0.0) / square * active
        coefficients = [coefficients[m] - removed * picks[m] for m in range(tasks)]
    weights = [jnp.sum(coefficients[m], axis=0, keepdims=True) for m in range(tasks)]

    half = rows // 2

    def segment(zi, yi, part, which):
        size = half if which is None else half // 2
        first = dp_at(zi, yi) * rows + part * half + (0 if which is None else which * size)
        return out_ref.at[pl.ds(pl.multiple_of(first, size), size), :]

    def mix(index, carry):
        mixed = sum(weights[t] * grads[t, index] for t in range(tasks))
        out_ref[pl.ds(pl.multiple_of(me_d * rows + index * step, step), step), :] = mixed.astype(jnp.bfloat16)
        return carry
    lax.fori_loop(0, blocks, mix, 0)

    def item(i):
        return (y, i) if i < 2 else (1 - y, 1)

    def hop(i, way, h, source=True):
        sign = 1 - 2 * way
        yi, part = item(i)
        which = way if h == far else None
        ref = segment(zof(-sign * (h - 1)), yi, part, which)
        return remote(ref, ref, ns_sem.at[i, way, h], nr_sem.at[i, way, h], (me_t, dp_at(zof(sign), y)))

    def cross(index, zi, part, which):
        ref = segment(zi, y, part, which)
        return remote(ref, ref, ms_sem.at[index], mr_sem.at[index], partner)

    zcopies, ycopies = [], []

    def go(copy, group):
        copy.start()
        group.append(copy)
        return copy

    got = {}
    second = go(cross(0, z, 1, None), ycopies)
    for i in (0, 1):
        for way in (0, 1):
            got[i, way, 1] = go(hop(i, way, 1), zcopies)
    go(cross(1, z, 0, None), ycopies)
    count = 2

    def onward(i, h):
        nonlocal count
        for way in (0, 1):
            got[i, way, h].wait_recv()
            if h < far:
                got[i, way, h + 1] = go(hop(i, way, h + 1), zcopies)
            if i == 0:
                sign = 1 - 2 * way
                go(cross(count, zof(-sign * h), 0, way if h == far else None), ycopies)
                count += 1

    onward(0, 1)
    second.wait_recv()
    for way in (0, 1):
        got[2, way, 1] = go(hop(2, way, 1), zcopies)
    onward(1, 1)
    for h in range(2, far + 1):
        onward(0, h)
        onward(2, h - 1)
        onward(1, h)
    onward(2, far)
    for copy in ycopies[1:]:
        copy.wait_recv()
    for copy in [*ycopies, *zcopies]:
        copy.wait_send()
    for j in range(1, tasks):
        c_remote(j).wait_send()

    def sent(copies):
        for copy in copies:
            copy.wait_send()

    def close_a(u):
        sent(ya(u))
        for m, sign, _, _ in messages(u):
            sent(za(u, m, sign))

    def close_b(u):
        sent(yb(u))
        for m, sign, _, _ in messages(u):
            sent(zb(u, m, sign))
    each(sum(first_y), close_a)
    each(sum(first_z), close_b)


def solution(mesh):
    tasks, ndp = mesh.shape["task"], mesh.shape["dp"]
    nz = ndp // 2

    def on_device(inputs, cotangent, task_order, conflict_flags):
        cot = cotangent[0]
        tokens = cot.shape[0]
        rows = inputs.shape[1] // ndp
        step = min(rows, 128)
        blocks = rows // step
        width = cot.shape[1] // tasks
        na = sum(plan(tasks, blocks))
        nb = tasks * blocks - na
        vmem, dma = pltpu.VMEM, pltpu.SemaphoreType.DMA
        f32, i16, bf16 = jnp.float32, jnp.int16, jnp.bfloat16
        hops = max(nz - 1, 1)
        scratch = [
            vmem(inputs.shape, bf16), vmem((ndp * blocks, step, tokens), bf16), vmem((tasks, tokens, width), bf16),
            vmem((na, nz, step, width), i16), vmem((na, nz, 1, width), f32),
            vmem((na, nz, step, width), i16), vmem((na, nz, 1, width), f32),
            vmem((na, hops, step, width), i16), vmem((na, hops, 1, width), f32),
            vmem((na, hops, step, width), i16), vmem((na, hops, 1, width), f32),
            vmem((na, nz, step, width), f32),
            vmem((nb, step, width), i16), vmem((nb, 1, width), f32),
            vmem((nb, step, width), i16), vmem((nb, 1, width), f32),
            vmem((nb, hops, 2, step, width), i16), vmem((nb, hops, 2, 1, width), f32),
            vmem((nb, hops, 2, step, width), i16), vmem((nb, hops, 2, 1, width), f32),
            vmem((nb, 2, step, width), f32),
            vmem((tasks, blocks, step, width), f32),
            vmem((8, 128), f32), vmem((ndp, 8, 128), f32), vmem((8, 128), f32), vmem((tasks, 8, 128), f32),
            dma((ndp,)), dma, dma((tasks,)), dma((tasks,)),
            dma((na, 2)), dma((na, 2)), dma((na, hops, 2)), dma((na, hops, 2)),
            dma((nb, 2)), dma((nb, 2)), dma((nb, hops, 2)), dma((nb, hops, 2)),
            dma((ndp,)), dma((ndp,)), dma((tasks,)), dma((tasks,)),
            dma((3, 2, nz)), dma((3, 2, nz)), dma((nz + 2,)), dma((nz + 2,)),
        ]
        smem = pl.BlockSpec(memory_space=pltpu.SMEM)
        whole = pl.BlockSpec(memory_space=pltpu.VMEM)
        hbm = pl.BlockSpec(memory_space=pl.ANY)
        return pl.pallas_call(
            functools.partial(kernel, tasks, ndp, blocks),
            out_shape=jax.ShapeDtypeStruct((inputs.shape[1], width), jnp.bfloat16),
            in_specs=[smem, smem, hbm, hbm],
            out_specs=whole,
            scratch_shapes=scratch,
            compiler_params=pltpu.CompilerParams(collective_id=0, has_side_effects=True,
                                                 vmem_limit_bytes=60 * 1024 * 1024),
        )(task_order, conflict_flags, inputs, cot)

    return jax.shard_map(
        on_device, mesh=mesh,
        in_specs=(P("dp", None), P("task", "dp", None), P(), P()),
        out_specs=P(None, "task"), check_vma=False,
    )
```

```python
import functools

import jax
import jax.numpy as jnp
from jax import lax
from jax.experimental import pallas as pl
from jax.experimental.pallas import tpu as pltpu
from jax.sharding import PartitionSpec as P

MESH = pl.DeviceIdType.MESH
TOP = 32767.0
LAG = 3
PIECES = 8
CROSSING = 6


def coded(tile):
    high = jnp.maximum(jnp.max(jnp.abs(tile), axis=0, keepdims=True), 1e-30)
    code = jnp.round(tile * (TOP / high)).astype(jnp.int32).astype(jnp.int16)
    return code, high * (1.0 / TOP)


def decoded(code, scale):
    return code.astype(jnp.int32).astype(jnp.float32) * scale


def shares(blocks):
    low = blocks * 7 // 16
    return low, blocks * 7 // 8 - low


def kernel(tasks, ndp, blocks, order_ref, flags_ref, x_hbm, c_hbm, out_ref,
           x_ref, cots, acc, ysend_a, yscale_a, yrecv_a, yrscale_a, zsend_a, zscale_a, zrecv_a, zrscale_a,
           ysend_b, yscale_b, yrecv_b, yrscale_b, zsend_b, zscale_b, zrecv_b, zrscale_b,
           grads, gram_own, gram_dp, gram_mid, gram_task,
           x_sem, c_sem, cs_sem, cr_sem,
           yas_sem, yar_sem, zas_sem, zar_sem, ybs_sem, ybr_sem, zbs_sem, zbr_sem,
           gs_sem, gr_sem, hs_sem, hr_sem, zgs_sem, zgr_sem, ygs_sem, ygr_sem, yhs_sem, yhr_sem):
    nz = ndp // 2
    pairs_of = tasks // 2
    me_t = lax.axis_index("task")
    me_d = lax.axis_index("dp")
    z = me_d // 2
    y = me_d % 2
    step = acc.shape[1]
    width = cots.shape[2]
    rows = step * blocks
    low_b, high_b = shares(blocks)
    low_a, high_a = blocks - high_b, blocks - low_b
    pair_b, pair_a = low_b + high_b, low_a + high_a
    units_a, units_b = pair_a * pairs_of, pair_b * pairs_of
    at_end = (z == 0) | (z == nz - 1)

    def dp_at(zi, yi):
        return zi * 2 + yi

    def mate(j, way):
        return lax.rem(me_t // 2 + way * (j // 2) + pairs_of, pairs_of) * 2 + lax.rem(me_t % 2 + j % 2, 2)

    def place_a(u):
        r = u % pair_a
        return u // pair_a * 2 + r // high_a, r % high_a

    def place_b(u):
        r = u % pair_b
        odd = (r + high_b - low_b) // high_b
        return u // pair_b * 2 + odd, r - odd * low_b + high_a - odd * (high_a - low_a)

    partner = (me_t, dp_at(z, 1 - y))

    def remote(src, dst, s, r, device):
        return pltpu.make_async_remote_copy(src_ref=src, dst_ref=dst, send_sem=s, recv_sem=r,
                                            device_id=device, device_id_type=MESH)

    c_copy = pltpu.make_async_copy(c_hbm.at[:, pl.ds(pl.multiple_of(me_t * width, width), width)], cots.at[0], c_sem)
    c_copy.start()
    x_copies = []
    for d in range(4):
        part = pl.ds(d * rows, rows)
        x_copies.append(pltpu.make_async_copy(x_hbm.at[:, part], x_ref.at[:, part], x_sem.at[d]))
        x_copies[-1].start()

    barrier = pltpu.get_barrier_semaphore()
    for k in range(1, ndp):
        pl.semaphore_signal(barrier, inc=1, device_id=(me_t, lax.rem(me_d + k, ndp)), device_id_type=MESH)
    for k in range(1, tasks):
        pl.semaphore_signal(barrier, inc=1, device_id=(lax.rem(me_t + k, tasks), me_d), device_id_type=MESH)
    pl.semaphore_wait(barrier, ndp + tasks - 2)

    def c_remote(j):
        peer = mate(j, 1)
        return remote(c_hbm.at[:, pl.ds(pl.multiple_of(peer * width, width), width)], cots.at[j],
                      cs_sem.at[j], cr_sem.at[j], (peer, me_d))

    for j in range(1, tasks):
        c_remote(j).start()
    c_copy.wait()
    for copy in x_copies:
        copy.wait()

    def product(j, block, end, yi):
        first = pl.multiple_of((dp_at(end, yi) * blocks + block) * step, step)
        return lax.dot_general(x_ref[:, pl.ds(first, step)], cots[j], (((0,), (0,)), ((), ())),
                               preferred_element_type=jnp.float32)

    def hop(end):
        return z if end else nz - 1 - z

    def ahead(end):
        return (me_t, dp_at(jnp.clip(z + (1 if end else -1), 0, nz - 1), y))

    def ya(u, end):
        return (remote(ysend_a.at[u, end], yrecv_a.at[u, end], yas_sem.at[u, end, 0], yar_sem.at[u, end, 0], partner),
                remote(yscale_a.at[u, end], yrscale_a.at[u, end], yas_sem.at[u, end, 1], yar_sem.at[u, end, 1], partner))

    def yb(u):
        return (remote(ysend_b.at[u], yrecv_b.at[u], ybs_sem.at[u, 0], ybr_sem.at[u, 0], partner),
                remote(yscale_b.at[u], yrscale_b.at[u], ybs_sem.at[u, 1], ybr_sem.at[u, 1], partner))

    def za(u, end):
        device = ahead(end)
        return (remote(zsend_a.at[u, end], zrecv_a.at[u, end], zas_sem.at[u, end, 0], zar_sem.at[u, end, 0], device),
                remote(zscale_a.at[u, end], zrscale_a.at[u, end], zas_sem.at[u, end, 1], zar_sem.at[u, end, 1], device))

    def zb(i, end):
        device = ahead(end)
        return (remote(zsend_b.at[i, end], zrecv_b.at[i, end], zbs_sem.at[i, end, 0], zbr_sem.at[i, end, 0], device),
                remote(zscale_b.at[i, end], zrscale_b.at[i, end], zbs_sem.at[i, end, 1], zbr_sem.at[i, end, 1], device))

    def start(copies):
        for copy in copies:
            copy.start()

    def arrive(copies):
        for copy in copies:
            copy.wait_recv()

    def each(first, last, body):
        if last > first:
            lax.fori_loop(first, last, lambda i, carry: (body(i), carry)[1], 0)

    def a_y(j, i):
        u = j // 2 * pair_a + j % 2 * high_a + i
        for end in (0, 1):
            code, scale = coded(product(j, i, end, 1 - y))
            ysend_a[u, end] = code
            yscale_a[u, end] = scale
            start(ya(u, end))

    def b_z(i, end):
        u, p = i // 2, i % 2
        j, block = place_b(u)
        acc[end] = product(j, block, end, lax.rem(1 - y + p, 2))

        @pl.when(hop(end) > 0)
        def _():
            arrive(zb(i, end))
            acc[end] = acc[end] + decoded(zrecv_b[i, end], zrscale_b[i, end])

        @pl.when(hop(end) < nz - 1)
        def _():
            code, scale = coded(acc[end])
            zsend_b[i, end] = code
            zscale_b[i, end] = scale
            start(zb(i, end))

        @pl.when((hop(end) == nz - 1) & (p == 0))
        def _():
            code, scale = coded(acc[end])
            ysend_b[u] = code
            yscale_b[u] = scale
            start(yb(u))

        @pl.when((hop(end) == nz - 1) & (p == 1))
        def _():
            grads[mate(j, -1), block] = acc[end]

    def a_z(u, end):
        j, block = place_a(u)
        total = product(j, block, end, y)
        arrive(ya(u, end))
        acc[end] = total + decoded(yrecv_a[u, end], yrscale_a[u, end])

        @pl.when(hop(end) > 0)
        def _():
            arrive(za(u, end))
            acc[end] = acc[end] + decoded(zrecv_a[u, end], zrscale_a[u, end])

        @pl.when(hop(end) < nz - 1)
        def _():
            code, scale = coded(acc[end])
            zsend_a[u, end] = code
            zscale_a[u, end] = scale
            start(za(u, end))

        @pl.when(hop(end) == nz - 1)
        def _():
            grads[mate(j, -1), block] = acc[end]

    items_b = 2 * units_b

    def advance(s):
        for end in (1, 0):
            at = s - LAG * hop(end)

            @pl.when((at >= 0) & (at < items_b))
            def _():
                b_z(at, end)

            @pl.when((at >= items_b) & (at < items_b + units_a))
            def _():
                a_z(at - items_b, end)

    s = 0
    for j in range(tasks):
        if j:
            c_remote(j).wait_recv()
        steps = 2 * (high_b if j % 2 else low_b)
        count = low_a if j % 2 else high_a
        several = -(-count // steps)

        def both(i, first=s, j=j, count=count, several=several):
            for q in range(several):
                @pl.when((i - first) * several + q < count)
                def _():
                    a_y(j, (i - first) * several + q)
            advance(i)
        each(s, s + steps, both)
        s += steps
    each(s, items_b + units_a + LAG * (nz - 1), advance)

    def finish_b(u):
        j, block = place_b(u)
        arrive(yb(u))
        task = mate(j, -1)
        grads[task, block] = grads[task, block] + decoded(yrecv_b[u], yrscale_b[u])

    end_of = z // max(nz - 1, 1)
    mine = dp_at(end_of, y) * rows

    def weigh():
        each(0, units_b, finish_b)
        pairs = [(s, t) for s in range(tasks) for t in range(s, tasks)]

        def products(index, sums):
            held = [grads[t, index] for t in range(tasks)]
            return tuple(total + jnp.sum((held[s] * held[t]).reshape(step // 8, 8, width), axis=0)
                         for total, (s, t) in zip(sums, pairs))

        sums = lax.fori_loop(0, blocks, products, tuple(jnp.zeros((8, width), jnp.float32) for _ in pairs))
        line = lax.broadcasted_iota(jnp.int32, (8, 128), 0)
        lane = lax.broadcasted_iota(jnp.int32, (8, 128), 1)
        gram = jnp.zeros((8, 128), jnp.float32)
        for total, (s, t) in zip(sums, pairs):
            value = jnp.sum(jnp.sum(total, axis=0, keepdims=True), axis=1, keepdims=True)
            here = ((line == s) & (lane == t)) | ((line == t) & (lane == s))
            gram = gram + jnp.where(here, value, 0.0)

        def swap(value, buffer_own, buffer, count, s_sem, r_sem, device):
            buffer_own[...] = value
            copies = [remote(buffer_own, buffer.at[k], s_sem.at[k], r_sem.at[k], device(k)) for k in range(1, count)]
            start(copies)
            for k, copy in enumerate(copies, 1):
                copy.wait_recv()
                value = value + buffer[k]
            for copy in copies:
                copy.wait_send()
            return value

        def other(k):
            return (me_t, dp_at(z if k % 2 == k else nz - 1 - z, y if k % 2 == 0 else 1 - y))

        gram = swap(gram, gram_own, gram_dp, 4, gs_sem, gr_sem, other)
        gram = swap(gram, gram_mid, gram_task, tasks, hs_sem, hr_sem, lambda k: (lax.rem(me_t + k, tasks), me_d))

        cols = [jnp.sum(jnp.where(lane == m, gram, 0.0), axis=1, keepdims=True) for m in range(tasks)]
        entry = lambda column, i: jnp.sum(jnp.where(line[:, :1] == i, column, 0.0), axis=0, keepdims=True)
        row = line[:, :1]
        coefficients = [(row == m).astype(jnp.float32) for m in range(tasks)]
        flag_cols = []
        for m in range(tasks):
            column = jnp.zeros((8, 1), jnp.float32)
            for i in range(tasks):
                column = column + jnp.where(row == i, flags_ref[i, m].astype(jnp.float32), 0.0)
            flag_cols.append(column)
        for position in range(tasks):
            target = order_ref[position]
            picks = [jnp.where(target == m, 1.0, 0.0) for m in range(tasks)]
            column = sum(cols[m] * picks[m] for m in range(tasks))
            dots = sum(coefficients[m] * entry(column, m) for m in range(tasks))
            square = sum(entry(column, m) * picks[m] for m in range(tasks))
            active = sum(flag_cols[m] * picks[m] for m in range(tasks)) * jnp.where(row == target, 0.0, 1.0)
            removed = jnp.minimum(dots, 0.0) / square * active
            coefficients = [coefficients[m] - removed * picks[m] for m in range(tasks)]
        weights = [jnp.sum(coefficients[m], axis=0, keepdims=True) for m in range(tasks)]

        def mix(index, carry):
            mixed = sum(weights[t] * grads[t, index] for t in range(tasks))
            out_ref[pl.ds(pl.multiple_of(mine + index * step, step), step), :] = mixed.astype(jnp.bfloat16)
            return carry
        lax.fori_loop(0, blocks, mix, 0)

    pl.when(at_end)(weigh)

    size = rows // PIECES
    chunks = 2 * PIECES - CROSSING

    def segment(end, yi, chunk):
        return out_ref.at[pl.ds(pl.multiple_of(dp_at(end, yi) * rows + chunk * size, size), size), :]

    def along(end, i):
        chunk = jnp.where(i < PIECES, i, i - PIECES + CROSSING)
        ref = segment(end, jnp.where(i < PIECES, y, 1 - y), chunk)
        return remote(ref, ref, zgs_sem.at[end, i], zgr_sem.at[end, i], ahead(1 - end))

    def over(end, i):
        ref = segment(end, y, i)
        return remote(ref, ref, ygs_sem.at[end, i], ygr_sem.at[end, i], partner)

    def early(i):
        ref = segment(end_of, y, i)
        return remote(ref, ref, yhs_sem.at[i], yhr_sem.at[i], partner)

    @pl.when(at_end)
    def _():
        each(CROSSING, PIECES, lambda i: early(i).start())

    def spread(s):
        for end in (0, 1):
            far = hop(1 - end)
            i = s - LAG * far

            @pl.when((i >= 0) & (i < chunks))
            def _():
                @pl.when(far > 0)
                def _():
                    along(end, i).wait_recv()

                @pl.when((far == 0) & (i >= PIECES))
                def _():
                    early(i - PIECES + CROSSING).wait_recv()

                @pl.when(far < nz - 1)
                def _():
                    along(end, i).start()

                @pl.when(i < CROSSING)
                def _():
                    over(end, i).start()

    each(0, chunks + LAG * (nz - 1), spread)

    def close(i):
        for end in (0, 1):
            over(end, i).wait_recv()
            over(end, i).wait_send()
    each(0, CROSSING, close)

    @pl.when(at_end)
    def _():
        each(CROSSING, PIECES, lambda i: early(i).wait_send())

    for j in range(1, tasks):
        c_remote(j).wait_send()

    def sent(copies):
        for copy in copies:
            copy.wait_send()

    def close_y(u):
        for end in (0, 1):
            sent(ya(u, end))
    each(0, units_a, close_y)
    pl.when(at_end)(lambda: each(0, units_b, lambda u: sent(yb(u))))
    for end in (0, 1):
        @pl.when(hop(end) < nz - 1)
        def _():
            each(0, units_a, lambda u: sent(za(u, end)))
            each(0, items_b, lambda i: sent(zb(i, end)))
            each(0, chunks, lambda i: along(1 - end, i).wait_send())


def solution(mesh):
    tasks, ndp = mesh.shape["task"], mesh.shape["dp"]

    def on_device(inputs, cotangent, task_order, conflict_flags):
        cot = cotangent[0]
        tokens = cot.shape[0]
        rows = inputs.shape[1] // 4
        step = min(rows, 128)
        blocks = rows // step
        width = cot.shape[1] // tasks
        nb = sum(shares(blocks)) * (tasks // 2)
        na = tasks * blocks - nb
        vmem, dma = pltpu.VMEM, pltpu.SemaphoreType.DMA
        f32, i16, bf16 = jnp.float32, jnp.int16, jnp.bfloat16
        code, scale = (step, width), (1, width)
        chunks = 2 * PIECES - CROSSING
        scratch = [
            vmem(inputs.shape, bf16), vmem((tasks, tokens, width), bf16), vmem((2, step, width), f32),
            vmem((na, 2, *code), i16), vmem((na, 2, *scale), f32), vmem((na, 2, *code), i16), vmem((na, 2, *scale), f32),
            vmem((na, 2, *code), i16), vmem((na, 2, *scale), f32), vmem((na, 2, *code), i16), vmem((na, 2, *scale), f32),
            vmem((nb, *code), i16), vmem((nb, *scale), f32), vmem((nb, *code), i16), vmem((nb, *scale), f32),
            vmem((2 * nb, 2, *code), i16), vmem((2 * nb, 2, *scale), f32),
            vmem((2 * nb, 2, *code), i16), vmem((2 * nb, 2, *scale), f32),
            vmem((tasks, blocks, step, width), f32),
            vmem((8, 128), f32), vmem((4, 8, 128), f32), vmem((8, 128), f32), vmem((tasks, 8, 128), f32),
            dma((4,)), dma, dma((tasks,)), dma((tasks,)),
            dma((na, 2, 2)), dma((na, 2, 2)), dma((na, 2, 2)), dma((na, 2, 2)),
            dma((nb, 2)), dma((nb, 2)), dma((2 * nb, 2, 2)), dma((2 * nb, 2, 2)),
            dma((4,)), dma((4,)), dma((tasks,)), dma((tasks,)),
            dma((2, chunks)), dma((2, chunks)), dma((2, CROSSING)), dma((2, CROSSING)), dma((PIECES,)), dma((PIECES,)),
        ]
        smem = pl.BlockSpec(memory_space=pltpu.SMEM)
        whole = pl.BlockSpec(memory_space=pltpu.VMEM)
        hbm = pl.BlockSpec(memory_space=pl.ANY)
        return pl.pallas_call(
            functools.partial(kernel, tasks, ndp, blocks),
            out_shape=jax.ShapeDtypeStruct((inputs.shape[1], width), jnp.bfloat16),
            in_specs=[smem, smem, hbm, hbm],
            out_specs=whole,
            scratch_shapes=scratch,
            compiler_params=pltpu.CompilerParams(collective_id=0, has_side_effects=True,
                                                 vmem_limit_bytes=60 * 1024 * 1024),
        )(task_order, conflict_flags, inputs, cot)

    return jax.shard_map(
        on_device, mesh=mesh,
        in_specs=(P("dp", None), P("task", "dp", None), P(), P()),
        out_specs=P(None, "task"), check_vma=False,
    )
```

```python
import functools

import jax
import jax.numpy as jnp
from jax import lax
from jax.experimental import pallas as pl
from jax.experimental.pallas import tpu as pltpu
from jax.sharding import PartitionSpec as P

MESH = pl.DeviceIdType.MESH
TOP = 32767.0
LAG = 3
SHARE = 12
REACH = 5
PIECES = 16
CROSSING = 12


def coded(tile):
    high = jnp.maximum(jnp.max(jnp.abs(tile), axis=0, keepdims=True), 1e-30)
    code = jnp.round(tile * (TOP / high)).astype(jnp.int32).astype(jnp.int16)
    return code, high * (1.0 / TOP)


def decoded(code, scale):
    return code.astype(jnp.int32).astype(jnp.float32) * scale


def shares(blocks):
    low = blocks * SHARE // 32
    return low, blocks * SHARE // 16 - low


def kernel(tasks, ndp, blocks, order_ref, flags_ref, x_hbm, c_hbm, out_ref,
           x_ref, cots, acc, ysend_a, yscale_a, yrecv_a, yrscale_a, zsend_a, zscale_a, zrecv_a, zrscale_a,
           ysend_b, yscale_b, yrecv_b, yrscale_b, zsend_b, zscale_b, zrecv_b, zrscale_b,
           grads, gram_own, gram_all,
           x_sem, c_sem, cs_sem, cr_sem,
           yas_sem, yar_sem, zas_sem, zar_sem, ybs_sem, ybr_sem, zbs_sem, zbr_sem,
           gs_sem, gr_sem, zgs_sem, zgr_sem, ygs_sem, ygr_sem, yhs_sem, yhr_sem):
    nz = ndp // 2
    pairs_of = tasks // 2
    me_t = lax.axis_index("task")
    me_d = lax.axis_index("dp")
    z = me_d // 2
    y = me_d % 2
    step = acc.shape[1]
    width = cots.shape[2]
    rows = step * blocks
    low_b, high_b = shares(blocks)
    low_a, high_a = blocks - high_b, blocks - low_b
    pair_b, pair_a = low_b + high_b, low_a + high_a
    units_a, units_b = pair_a * pairs_of, pair_b * pairs_of
    at_end = (z == 0) | (z == nz - 1)

    def dp_at(zi, yi):
        return zi * 2 + yi

    def mate(j, way):
        return lax.rem(me_t // 2 + way * (j // 2) + pairs_of, pairs_of) * 2 + lax.rem(me_t % 2 + j % 2, 2)

    def place_a(u):
        r = u % pair_a
        return u // pair_a * 2 + r // high_a, r % high_a

    def place_b(u):
        r = u % pair_b
        odd = (r + high_b - low_b) // high_b
        return u // pair_b * 2 + odd, r - odd * low_b + high_a - odd * (high_a - low_a)

    partner = (me_t, dp_at(z, 1 - y))

    def remote(src, dst, s, r, device):
        return pltpu.make_async_remote_copy(src_ref=src, dst_ref=dst, send_sem=s, recv_sem=r,
                                            device_id=device, device_id_type=MESH)

    c_copy = pltpu.make_async_copy(c_hbm.at[:, pl.ds(pl.multiple_of(me_t * width, width), width)], cots.at[0], c_sem)
    c_copy.start()
    x_copies = []
    for d in range(4):
        part = pl.ds(d * rows, rows)
        x_copies.append(pltpu.make_async_copy(x_hbm.at[:, part], x_ref.at[:, part], x_sem.at[d]))
        x_copies[-1].start()

    def hop(end):
        return z if end else nz - 1 - z

    def ahead(end):
        return (me_t, dp_at(jnp.clip(z + (1 if end else -1), 0, nz - 1), y))

    barrier = pltpu.get_barrier_semaphore()
    pl.semaphore_signal(barrier, inc=1, device_id=partner, device_id_type=MESH)
    for k in range(1, tasks):
        pl.semaphore_signal(barrier, inc=1, device_id=(lax.rem(me_t + k, tasks), me_d), device_id_type=MESH)
    for end in (0, 1):
        @pl.when(hop(end) < nz - 1)
        def _():
            pl.semaphore_signal(barrier, inc=1, device_id=ahead(end), device_id_type=MESH)
    pl.semaphore_wait(barrier, tasks + jnp.where(z > 0, 1, 0) + jnp.where(z < nz - 1, 1, 0))

    def c_remote(j):
        peer = mate(j, 1)
        return remote(c_hbm.at[:, pl.ds(pl.multiple_of(peer * width, width), width)], cots.at[j],
                      cs_sem.at[j], cr_sem.at[j], (peer, me_d))

    for j in range(1, tasks):
        c_remote(j).start()
    c_copy.wait()
    for copy in x_copies:
        copy.wait()

    def product(j, block, end, yi):
        first = pl.multiple_of((dp_at(end, yi) * blocks + block) * step, step)
        return lax.dot_general(x_ref[:, pl.ds(first, step)], cots[j], (((0,), (0,)), ((), ())),
                               preferred_element_type=jnp.float32)

    def ya(u, end):
        return (remote(ysend_a.at[u, end], yrecv_a.at[u, end], yas_sem.at[u, end, 0], yar_sem.at[u, end, 0], partner),
                remote(yscale_a.at[u, end], yrscale_a.at[u, end], yas_sem.at[u, end, 1], yar_sem.at[u, end, 1], partner))

    def yb(u):
        return (remote(ysend_b.at[u], yrecv_b.at[u], ybs_sem.at[u, 0], ybr_sem.at[u, 0], partner),
                remote(yscale_b.at[u], yrscale_b.at[u], ybs_sem.at[u, 1], ybr_sem.at[u, 1], partner))

    def za(u, end):
        device = ahead(end)
        return (remote(zsend_a.at[u, end], zrecv_a.at[u, end], zas_sem.at[u, end, 0], zar_sem.at[u, end, 0], device),
                remote(zscale_a.at[u, end], zrscale_a.at[u, end], zas_sem.at[u, end, 1], zar_sem.at[u, end, 1], device))

    def zb(i, end):
        device = ahead(end)
        return (remote(zsend_b.at[i, end], zrecv_b.at[i, end], zbs_sem.at[i, end, 0], zbr_sem.at[i, end, 0], device),
                remote(zscale_b.at[i, end], zrscale_b.at[i, end], zbs_sem.at[i, end, 1], zbr_sem.at[i, end, 1], device))

    def start(copies):
        for copy in copies:
            copy.start()

    def arrive(copies):
        for copy in copies:
            copy.wait_recv()

    def each(first, last, body):
        if last > first:
            lax.fori_loop(first, last, lambda i, carry: (body(i), carry)[1], 0)

    def a_y(j, i):
        u = j // 2 * pair_a + j % 2 * high_a + i
        for end in (0, 1):
            code, scale = coded(product(j, i, end, 1 - y))
            ysend_a[u, end] = code
            yscale_a[u, end] = scale
            start(ya(u, end))

    def b_z(i, end):
        u, p = i // 2, i % 2
        j, block = place_b(u)
        acc[end] = product(j, block, end, lax.rem(1 - y + p, 2))

        @pl.when(hop(end) > 0)
        def _():
            arrive(zb(i, end))
            acc[end] = acc[end] + decoded(zrecv_b[i, end], zrscale_b[i, end])

        @pl.when(hop(end) < nz - 1)
        def _():
            code, scale = coded(acc[end])
            zsend_b[i, end] = code
            zscale_b[i, end] = scale
            start(zb(i, end))

        @pl.when((hop(end) == nz - 1) & (p == 0))
        def _():
            code, scale = coded(acc[end])
            ysend_b[u] = code
            yscale_b[u] = scale

            @pl.when(i >= held)
            def _():
                start(yb(u))

        @pl.when((hop(end) == nz - 1) & (p == 1))
        def _():
            grads[mate(j, -1), block] = acc[end]

    def a_z(u, end):
        j, block = place_a(u)
        total = product(j, block, end, y)
        arrive(ya(u, end))
        acc[end] = total + decoded(yrecv_a[u, end], yrscale_a[u, end])

        @pl.when(hop(end) > 0)
        def _():
            arrive(za(u, end))
            acc[end] = acc[end] + decoded(zrecv_a[u, end], zrscale_a[u, end])

        @pl.when(hop(end) < nz - 1)
        def _():
            code, scale = coded(acc[end])
            zsend_a[u, end] = code
            zscale_a[u, end] = scale
            start(za(u, end))

        @pl.when(hop(end) == nz - 1)
        def _():
            grads[mate(j, -1), block] = acc[end]

    items_b = 2 * units_b
    held = max(items_b - LAG * (nz - 1), 0)

    def advance(s):
        for end in (1, 0):
            at = s - LAG * hop(end)

            @pl.when((at >= 0) & (at < items_b))
            def _():
                b_z(at, end)

            @pl.when((at >= items_b) & (at < items_b + units_a))
            def _():
                a_z(at - items_b, end)

    s = 0
    for j in range(tasks):
        if j:
            c_remote(j).wait_recv()
        steps = 2 * (high_b if j % 2 else low_b)
        count = low_a if j % 2 else high_a
        several = -(-count // steps)

        def both(i, first=s, j=j, count=count, several=several):
            for q in range(several):
                @pl.when((i - first) * several + q < count)
                def _():
                    a_y(j, (i - first) * several + q)
            advance(i)
        each(s, s + steps, both)
        s += steps
    pl.when(at_end)(lambda: each(0, -(-held // 2), lambda u: start(yb(u))))
    each(s, items_b + units_a + LAG * (nz - 1), advance)

    def finish_b(u):
        j, block = place_b(u)
        arrive(yb(u))
        task = mate(j, -1)
        grads[task, block] = grads[task, block] + decoded(yrecv_b[u], yrscale_b[u])

    end_of = z // max(nz - 1, 1)
    mine = dp_at(end_of, y) * rows

    def weigh():
        each(0, units_b, finish_b)
        pairs = [(s, t) for s in range(tasks) for t in range(s, tasks)]

        def products(index, sums):
            held = [grads[t, index] for t in range(tasks)]
            return tuple(total + jnp.sum((held[s] * held[t]).reshape(step // 8, 8, width), axis=0)
                         for total, (s, t) in zip(sums, pairs))

        sums = lax.fori_loop(0, blocks, products, tuple(jnp.zeros((8, width), jnp.float32) for _ in pairs))
        line = lax.broadcasted_iota(jnp.int32, (8, 128), 0)
        lane = lax.broadcasted_iota(jnp.int32, (8, 128), 1)
        gram = jnp.zeros((8, 128), jnp.float32)
        for total, (s, t) in zip(sums, pairs):
            value = jnp.sum(jnp.sum(total, axis=0, keepdims=True), axis=1, keepdims=True)
            here = ((line == s) & (lane == t)) | ((line == t) & (lane == s))
            gram = gram + jnp.where(here, value, 0.0)

        def peer(k):
            end = k // 2 % 2
            return (lax.rem(me_t + k // 4, tasks), dp_at(nz - 1 - z if end else z, 1 - y if k % 2 else y))

        gram_own[...] = gram
        copies = [remote(gram_own, gram_all.at[k], gs_sem.at[k], gr_sem.at[k], peer(k)) for k in range(1, 4 * tasks)]
        start(copies)
        for k, copy in enumerate(copies, 1):
            copy.wait_recv()
            gram = gram + gram_all[k]
        for copy in copies:
            copy.wait_send()

        cols = [jnp.sum(jnp.where(lane == m, gram, 0.0), axis=1, keepdims=True) for m in range(tasks)]
        entry = lambda column, i: jnp.sum(jnp.where(line[:, :1] == i, column, 0.0), axis=0, keepdims=True)
        row = line[:, :1]
        coefficients = [(row == m).astype(jnp.float32) for m in range(tasks)]
        flag_cols = []
        for m in range(tasks):
            column = jnp.zeros((8, 1), jnp.float32)
            for i in range(tasks):
                column = column + jnp.where(row == i, flags_ref[i, m].astype(jnp.float32), 0.0)
            flag_cols.append(column)
        for position in range(tasks):
            target = order_ref[position]
            picks = [jnp.where(target == m, 1.0, 0.0) for m in range(tasks)]
            column = sum(cols[m] * picks[m] for m in range(tasks))
            dots = sum(coefficients[m] * entry(column, m) for m in range(tasks))
            square = sum(entry(column, m) * picks[m] for m in range(tasks))
            active = sum(flag_cols[m] * picks[m] for m in range(tasks)) * jnp.where(row == target, 0.0, 1.0)
            removed = jnp.minimum(dots, 0.0) / square * active
            coefficients = [coefficients[m] - removed * picks[m] for m in range(tasks)]
        weights = [jnp.sum(coefficients[m], axis=0, keepdims=True) for m in range(tasks)]

        def mix(index, carry):
            mixed = sum(weights[t] * grads[t, index] for t in range(tasks))
            out_ref[pl.ds(pl.multiple_of(mine + index * step, step), step), :] = mixed.astype(jnp.bfloat16)
            return carry
        lax.fori_loop(0, blocks, mix, 0)

    pl.when(at_end)(weigh)

    size = rows // PIECES
    chunks = 2 * PIECES - CROSSING

    def segment(end, yi, chunk):
        return out_ref.at[pl.ds(pl.multiple_of(dp_at(end, yi) * rows + chunk * size, size), size), :]

    def along(end, i):
        chunk = jnp.where(i < PIECES, i, i - PIECES + CROSSING)
        ref = segment(end, jnp.where(i < PIECES, y, 1 - y), chunk)
        return remote(ref, ref, zgs_sem.at[end, i], zgr_sem.at[end, i], ahead(1 - end))

    def over(end, i):
        ref = segment(end, y, i)
        return remote(ref, ref, ygs_sem.at[end, i], ygr_sem.at[end, i], partner)

    def early(i):
        ref = segment(end_of, y, i)
        return remote(ref, ref, yhs_sem.at[i], yhr_sem.at[i], partner)

    @pl.when(at_end)
    def _():
        each(CROSSING, PIECES, lambda i: early(i).start())

    def spread(s):
        for end in (0, 1):
            far = hop(1 - end)
            i = s - REACH * far

            @pl.when((i >= 0) & (i < chunks))
            def _():
                @pl.when(far > 0)
                def _():
                    along(end, i).wait_recv()

                @pl.when((far == 0) & (i >= PIECES))
                def _():
                    early(i - PIECES + CROSSING).wait_recv()

                @pl.when(far < nz - 1)
                def _():
                    along(end, i).start()

                @pl.when(i < CROSSING)
                def _():
                    over(end, i).start()

    each(0, chunks + REACH * (nz - 1), spread)

    def close(i):
        for end in (0, 1):
            over(end, i).wait_recv()
            over(end, i).wait_send()
    each(0, CROSSING, close)

    @pl.when(at_end)
    def _():
        each(CROSSING, PIECES, lambda i: early(i).wait_send())

    for j in range(1, tasks):
        c_remote(j).wait_send()

    def sent(copies):
        for copy in copies:
            copy.wait_send()

    def close_y(u):
        for end in (0, 1):
            sent(ya(u, end))
    each(0, units_a, close_y)
    pl.when(at_end)(lambda: each(0, units_b, lambda u: sent(yb(u))))
    for end in (0, 1):
        @pl.when(hop(end) < nz - 1)
        def _():
            each(0, units_a, lambda u: sent(za(u, end)))
            each(0, items_b, lambda i: sent(zb(i, end)))
            each(0, chunks, lambda i: along(1 - end, i).wait_send())


def solution(mesh):
    tasks, ndp = mesh.shape["task"], mesh.shape["dp"]

    def on_device(inputs, cotangent, task_order, conflict_flags):
        cot = cotangent[0]
        tokens = cot.shape[0]
        rows = inputs.shape[1] // 4
        step = min(rows, 128)
        blocks = rows // step
        width = cot.shape[1] // tasks
        nb = sum(shares(blocks)) * (tasks // 2)
        na = tasks * blocks - nb
        vmem, dma = pltpu.VMEM, pltpu.SemaphoreType.DMA
        f32, i16, bf16 = jnp.float32, jnp.int16, jnp.bfloat16
        code, scale = (step, width), (1, width)
        chunks = 2 * PIECES - CROSSING
        scratch = [
            vmem(inputs.shape, bf16), vmem((tasks, tokens, width), bf16), vmem((2, step, width), f32),
            vmem((na, 2, *code), i16), vmem((na, 2, *scale), f32), vmem((na, 2, *code), i16), vmem((na, 2, *scale), f32),
            vmem((na, 2, *code), i16), vmem((na, 2, *scale), f32), vmem((na, 2, *code), i16), vmem((na, 2, *scale), f32),
            vmem((nb, *code), i16), vmem((nb, *scale), f32), vmem((nb, *code), i16), vmem((nb, *scale), f32),
            vmem((2 * nb, 2, *code), i16), vmem((2 * nb, 2, *scale), f32),
            vmem((2 * nb, 2, *code), i16), vmem((2 * nb, 2, *scale), f32),
            vmem((tasks, blocks, step, width), f32),
            vmem((8, 128), f32), vmem((4 * tasks, 8, 128), f32),
            dma((4,)), dma, dma((tasks,)), dma((tasks,)),
            dma((na, 2, 2)), dma((na, 2, 2)), dma((na, 2, 2)), dma((na, 2, 2)),
            dma((nb, 2)), dma((nb, 2)), dma((2 * nb, 2, 2)), dma((2 * nb, 2, 2)),
            dma((4 * tasks,)), dma((4 * tasks,)),
            dma((2, chunks)), dma((2, chunks)), dma((2, CROSSING)), dma((2, CROSSING)), dma((PIECES,)), dma((PIECES,)),
        ]
        smem = pl.BlockSpec(memory_space=pltpu.SMEM)
        whole = pl.BlockSpec(memory_space=pltpu.VMEM)
        hbm = pl.BlockSpec(memory_space=pltpu.HBM)
        return pl.pallas_call(
            functools.partial(kernel, tasks, ndp, blocks),
            out_shape=jax.ShapeDtypeStruct((inputs.shape[1], width), jnp.bfloat16),
            in_specs=[smem, smem, hbm, hbm],
            out_specs=whole,
            scratch_shapes=scratch,
            compiler_params=pltpu.CompilerParams(collective_id=0, has_side_effects=True,
                                                 vmem_limit_bytes=44 * 1024 * 1024),
        )(*[pltpu.with_memory_space_constraint(v, pltpu.HBM) for v in (task_order, conflict_flags, inputs, cot)])

    return jax.shard_map(
        on_device, mesh=mesh,
        in_specs=(P("dp", None), P("task", "dp", None), P(), P()),
        out_specs=P(None, "task"), check_vma=False,
    )
```

```python
import functools

import jax
import jax.numpy as jnp
from jax import lax
from jax.experimental import pallas as pl
from jax.experimental.pallas import tpu as pltpu
from jax.sharding import PartitionSpec as P

MESH = pl.DeviceIdType.MESH
TOP = 32767.0
LAG = 3
SHARE = 12
REACH = 5
PIECES = 16
CROSSING = 12


def coded(tile):
    high = jnp.maximum(jnp.max(jnp.abs(tile), axis=0, keepdims=True), 1e-30)
    code = jnp.round(tile * (TOP / high)).astype(jnp.int32).astype(jnp.int16)
    return code, high * (1.0 / TOP)


def decoded(code, scale):
    return code.astype(jnp.int32).astype(jnp.float32) * scale


def shares(blocks):
    low = blocks * SHARE // 32
    return low, blocks * SHARE // 16 - low


def kernel(tasks, ndp, blocks, order_ref, flags_ref, x_hbm, c_hbm, out_ref,
           x_ref, cots, acc, ysend_a, yscale_a, yrecv_a, yrscale_a, zsend_a, zscale_a, zrecv_a, zrscale_a,
           ysend_b, yscale_b, yrecv_b, yrscale_b, zsend_b, zscale_b, zrecv_b, zrscale_b,
           grads, gram_own, gram_all,
           x_sem, c_sem, cs_sem, cr_sem,
           yas_sem, yar_sem, zas_sem, zar_sem, ybs_sem, ybr_sem, zbs_sem, zbr_sem,
           gs_sem, gr_sem, zgs_sem, zgr_sem, ygs_sem, ygr_sem, yhs_sem, yhr_sem):
    nz = ndp // 2
    pairs_of = tasks // 2
    me_t = lax.axis_index("task")
    me_d = lax.axis_index("dp")
    z = me_d // 2
    y = me_d % 2
    step = acc.shape[1]
    width = cots.shape[2]
    rows = step * blocks
    low_b, high_b = shares(blocks)
    low_a, high_a = blocks - high_b, blocks - low_b
    pair_b, pair_a = low_b + high_b, low_a + high_a
    units_a, units_b = pair_a * pairs_of, pair_b * pairs_of
    at_end = (z == 0) | (z == nz - 1)

    def dp_at(zi, yi):
        return zi * 2 + yi

    def mate(j, way):
        return lax.rem(me_t // 2 + way * (j // 2) + pairs_of, pairs_of) * 2 + lax.rem(me_t % 2 + j % 2, 2)

    def place_a(u):
        r = u % pair_a
        return u // pair_a * 2 + r // high_a, r % high_a

    def place_b(u):
        r = u % pair_b
        odd = (r + high_b - low_b) // high_b
        return u // pair_b * 2 + odd, r - odd * low_b + high_a - odd * (high_a - low_a)

    partner = (me_t, dp_at(z, 1 - y))

    def remote(src, dst, s, r, device):
        return pltpu.make_async_remote_copy(src_ref=src, dst_ref=dst, send_sem=s, recv_sem=r,
                                            device_id=device, device_id_type=MESH)

    c_copy = pltpu.make_async_copy(c_hbm.at[:, pl.ds(pl.multiple_of(me_t * width, width), width)], cots.at[0], c_sem)
    c_copy.start()
    x_copies = []
    for d in range(4):
        part = pl.ds(pl.multiple_of(dp_at(d % 2, 1 - y if d < 2 else y) * rows, rows), rows)
        x_copies.append(pltpu.make_async_copy(x_hbm.at[:, part], x_ref.at[:, part], x_sem.at[d]))
        x_copies[-1].start()

    def hop(end):
        return z if end else nz - 1 - z

    def ahead(end):
        return (me_t, dp_at(jnp.clip(z + (1 if end else -1), 0, nz - 1), y))

    barrier = pltpu.get_barrier_semaphore()
    pl.semaphore_signal(barrier, inc=1, device_id=partner, device_id_type=MESH)
    for k in range(1, tasks):
        pl.semaphore_signal(barrier, inc=1, device_id=(lax.rem(me_t + k, tasks), me_d), device_id_type=MESH)
    for end in (0, 1):
        @pl.when(hop(end) < nz - 1)
        def _():
            pl.semaphore_signal(barrier, inc=1, device_id=ahead(end), device_id_type=MESH)
    pl.semaphore_wait(barrier, tasks + jnp.where(z > 0, 1, 0) + jnp.where(z < nz - 1, 1, 0))

    def c_remote(j):
        peer = mate(j, 1)
        return remote(c_hbm.at[:, pl.ds(pl.multiple_of(peer * width, width), width)], cots.at[j],
                      cs_sem.at[j], cr_sem.at[j], (peer, me_d))

    for j in range(1, tasks):
        c_remote(j).start()
    c_copy.wait()
    for copy in x_copies[:2]:
        copy.wait()

    def product(j, block, end, yi):
        first = pl.multiple_of((dp_at(end, yi) * blocks + block) * step, step)
        return lax.dot_general(x_ref[:, pl.ds(first, step)], cots[j], (((0,), (0,)), ((), ())),
                               preferred_element_type=jnp.float32)

    def ya(u):
        return (remote(ysend_a.at[u], yrecv_a.at[u], yas_sem.at[u, 0], yar_sem.at[u, 0], partner),
                remote(yscale_a.at[u], yrscale_a.at[u], yas_sem.at[u, 1], yar_sem.at[u, 1], partner))

    def yb(u):
        return (remote(ysend_b.at[u], yrecv_b.at[u], ybs_sem.at[u, 0], ybr_sem.at[u, 0], partner),
                remote(yscale_b.at[u], yrscale_b.at[u], ybs_sem.at[u, 1], ybr_sem.at[u, 1], partner))

    def za(u, end):
        device = ahead(end)
        return (remote(zsend_a.at[u, end], zrecv_a.at[u, end], zas_sem.at[u, end, 0], zar_sem.at[u, end, 0], device),
                remote(zscale_a.at[u, end], zrscale_a.at[u, end], zas_sem.at[u, end, 1], zar_sem.at[u, end, 1], device))

    def zb(i, end):
        device = ahead(end)
        return (remote(zsend_b.at[i, end], zrecv_b.at[i, end], zbs_sem.at[i, end, 0], zbr_sem.at[i, end, 0], device),
                remote(zscale_b.at[i, end], zrscale_b.at[i, end], zbs_sem.at[i, end, 1], zbr_sem.at[i, end, 1], device))

    def start(copies):
        for copy in copies:
            copy.start()

    def arrive(copies):
        for copy in copies:
            copy.wait_recv()

    def each(first, last, body):
        if last > first:
            lax.fori_loop(first, last, lambda i, carry: (body(i), carry)[1], 0)

    def a_y(j, i):
        u = j // 2 * pair_a + j % 2 * high_a + i
        for end in (0, 1):
            code, scale = coded(product(j, i, end, 1 - y))
            ysend_a[u, end] = code
            yscale_a[u, end] = scale
        start(ya(u))

    def b_z(i, end):
        u, p = i // 2, i % 2
        j, block = place_b(u)
        acc[end] = product(j, block, end, lax.rem(1 - y + p, 2))

        @pl.when(hop(end) > 0)
        def _():
            arrive(zb(i, end))
            acc[end] = acc[end] + decoded(zrecv_b[i, end], zrscale_b[i, end])

        @pl.when(hop(end) < nz - 1)
        def _():
            code, scale = coded(acc[end])
            zsend_b[i, end] = code
            zscale_b[i, end] = scale
            start(zb(i, end))

        @pl.when((hop(end) == nz - 1) & (p == 0))
        def _():
            code, scale = coded(acc[end])
            ysend_b[u] = code
            yscale_b[u] = scale

            @pl.when(i >= held)
            def _():
                start(yb(u))

        @pl.when((hop(end) == nz - 1) & (p == 1))
        def _():
            grads[mate(j, -1), block] = acc[end]

    def a_z(u, end):
        j, block = place_a(u)
        acc[end] = product(j, block, end, y)

        @pl.when(hop(end) < hop(1 - end))
        def _():
            arrive(ya(u))
        acc[end] = acc[end] + decoded(yrecv_a[u, end], yrscale_a[u, end])

        @pl.when(hop(end) > 0)
        def _():
            arrive(za(u, end))
            acc[end] = acc[end] + decoded(zrecv_a[u, end], zrscale_a[u, end])

        @pl.when(hop(end) < nz - 1)
        def _():
            code, scale = coded(acc[end])
            zsend_a[u, end] = code
            zscale_a[u, end] = scale
            start(za(u, end))

        @pl.when(hop(end) == nz - 1)
        def _():
            grads[mate(j, -1), block] = acc[end]

    items_b = 2 * units_b
    held = max(items_b - LAG * (nz - 1), 0)

    def advance(s):
        for end in (1, 0):
            at = s - LAG * hop(end)

            @pl.when((at >= 0) & (at < items_b))
            def _():
                b_z(at, end)

            @pl.when((at >= items_b) & (at < items_b + units_a))
            def _():
                a_z(at - items_b, end)

    s = 0
    for j in range(tasks):
        if j:
            c_remote(j).wait_recv()
        steps = 2 * (high_b if j % 2 else low_b)
        count = low_a if j % 2 else high_a
        several = -(-count // steps)

        def both(i, first=s, j=j, count=count, several=several):
            for q in range(several):
                @pl.when((i - first) * several + q < count)
                def _():
                    a_y(j, (i - first) * several + q)
            advance(i)
        if j:
            each(s, s + steps, both)
        else:
            both(0)
            for copy in x_copies[2:]:
                copy.wait()
            each(1, steps, both)
        s += steps
    pl.when(at_end)(lambda: each(0, -(-held // 2), lambda u: start(yb(u))))
    each(s, items_b + units_a + LAG * (nz - 1), advance)

    def finish_b(u):
        j, block = place_b(u)
        arrive(yb(u))
        task = mate(j, -1)
        grads[task, block] = grads[task, block] + decoded(yrecv_b[u], yrscale_b[u])

    end_of = z // max(nz - 1, 1)
    mine = dp_at(end_of, y) * rows

    size = rows // PIECES
    chunks = 2 * PIECES - CROSSING

    def segment(end, yi, chunk):
        return out_ref.at[pl.ds(pl.multiple_of(dp_at(end, yi) * rows + chunk * size, size), size), :]

    def early(i):
        ref = segment(end_of, y, i)
        return remote(ref, ref, yhs_sem.at[i], yhr_sem.at[i], partner)

    def settle():
        def sent(copies):
            for copy in copies:
                copy.wait_send()

        for j in range(1, tasks):
            c_remote(j).wait_send()
        each(0, units_a, lambda u: sent(ya(u)))
        for end in (0, 1):
            @pl.when(hop(end) < nz - 1)
            def _():
                each(0, units_a, lambda u: sent(za(u, end)))
                each(0, items_b, lambda i: sent(zb(i, end)))

    pl.when(jnp.logical_not(at_end))(settle)

    def weigh():
        each(0, units_b, finish_b)
        pairs = [(s, t) for s in range(tasks) for t in range(s, tasks)]

        def products(index, sums):
            held = [grads[t, index] for t in range(tasks)]
            return tuple(total + jnp.sum((held[s] * held[t]).reshape(step // 8, 8, width), axis=0)
                         for total, (s, t) in zip(sums, pairs))

        sums = lax.fori_loop(0, blocks, products, tuple(jnp.zeros((8, width), jnp.float32) for _ in pairs))
        line = lax.broadcasted_iota(jnp.int32, (8, 128), 0)
        lane = lax.broadcasted_iota(jnp.int32, (8, 128), 1)
        spot = lane[:1]
        row = jnp.zeros((1, 128), jnp.float32)
        for place, total in enumerate(sums):
            value = jnp.sum(jnp.sum(total, axis=0, keepdims=True), axis=1, keepdims=True)
            row = row + jnp.where(spot == place, value, 0.0)

        def peer(k):
            end = k // 2 % 2
            return (lax.rem(me_t + k // 4, tasks), dp_at(nz - 1 - z if end else z, 1 - y if k % 2 else y))

        gram_own[...] = row
        copies = [remote(gram_own, gram_all.at[k], gs_sem.at[k], gr_sem.at[k], peer(k)) for k in range(1, 4 * tasks)]
        start(copies)
        settle()
        for u in range(units_b):
            for copy in yb(u):
                copy.wait_send()
        for k, copy in enumerate(copies, 1):
            copy.wait_recv()
            row = row + gram_all[k]

        gram = jnp.zeros((8, 128), jnp.float32)
        for place, (s, t) in enumerate(pairs):
            value = jnp.sum(jnp.where(spot == place, row, 0.0), axis=1, keepdims=True)
            here = ((line == s) & (lane == t)) | ((line == t) & (lane == s))
            gram = gram + jnp.where(here, value, 0.0)
        cols = [jnp.sum(jnp.where(lane == m, gram, 0.0), axis=1, keepdims=True) for m in range(tasks)]
        entry = lambda column, i: jnp.sum(jnp.where(line[:, :1] == i, column, 0.0), axis=0, keepdims=True)
        rank = line[:, :1]
        coefficients = [(rank == m).astype(jnp.float32) for m in range(tasks)]
        flag_cols = []
        for m in range(tasks):
            column = jnp.zeros((8, 1), jnp.float32)
            for i in range(tasks):
                column = column + jnp.where(rank == i, flags_ref[i, m].astype(jnp.float32), 0.0)
            flag_cols.append(column)
        for position in range(tasks):
            target = order_ref[position]
            picks = [jnp.where(target == m, 1.0, 0.0) for m in range(tasks)]
            column = sum(cols[m] * picks[m] for m in range(tasks))
            dots = sum(coefficients[m] * entry(column, m) for m in range(tasks))
            square = sum(entry(column, m) * picks[m] for m in range(tasks))
            active = sum(flag_cols[m] * picks[m] for m in range(tasks)) * jnp.where(rank == target, 0.0, 1.0)
            removed = jnp.minimum(dots, 0.0) / square * active
            coefficients = [coefficients[m] - removed * picks[m] for m in range(tasks)]
        weights = [jnp.sum(coefficients[m], axis=0, keepdims=True) for m in range(tasks)]

        def mix(index):
            mixed = sum(weights[t] * grads[t, index] for t in range(tasks))
            out_ref[pl.ds(pl.multiple_of(mine + index * step, step), step), :] = mixed.astype(jnp.bfloat16)

        first = CROSSING * blocks // PIECES
        each(first, blocks, mix)
        each(CROSSING, PIECES, lambda i: early(i).start())
        each(0, first, mix)
        for copy in copies:
            copy.wait_send()

    pl.when(at_end)(weigh)

    def along(end, i):
        chunk = jnp.where(i < PIECES, i, i - PIECES + CROSSING)
        ref = segment(end, jnp.where(i < PIECES, y, 1 - y), chunk)
        return remote(ref, ref, zgs_sem.at[end, i], zgr_sem.at[end, i], ahead(1 - end))

    def over(end, i):
        ref = segment(end, y, i)
        return remote(ref, ref, ygs_sem.at[end, i], ygr_sem.at[end, i], partner)

    def spread(s):
        for end in (0, 1):
            far = hop(1 - end)
            i = s - REACH * far

            @pl.when((i >= 0) & (i < chunks))
            def _():
                @pl.when(far > 0)
                def _():
                    along(end, i).wait_recv()

                @pl.when((far == 0) & (i >= PIECES))
                def _():
                    early(i - PIECES + CROSSING).wait_recv()

                @pl.when(far < nz - 1)
                def _():
                    along(end, i).start()

                @pl.when(i < CROSSING)
                def _():
                    over(end, i).start()

    each(0, chunks + REACH * (nz - 1), spread)

    def close(i):
        for end in (0, 1):
            over(end, i).wait_recv()
            over(end, i).wait_send()
    each(0, CROSSING, close)

    @pl.when(at_end)
    def _():
        each(CROSSING, PIECES, lambda i: early(i).wait_send())

    for end in (0, 1):
        @pl.when(hop(end) < nz - 1)
        def _():
            each(0, chunks, lambda i: along(1 - end, i).wait_send())


def solution(mesh):
    tasks, ndp = mesh.shape["task"], mesh.shape["dp"]

    def on_device(inputs, cotangent, task_order, conflict_flags):
        cot = cotangent[0]
        tokens = cot.shape[0]
        rows = inputs.shape[1] // 4
        step = min(rows, 128)
        blocks = rows // step
        width = cot.shape[1] // tasks
        nb = sum(shares(blocks)) * (tasks // 2)
        na = tasks * blocks - nb
        vmem, dma = pltpu.VMEM, pltpu.SemaphoreType.DMA
        f32, i16, bf16 = jnp.float32, jnp.int16, jnp.bfloat16
        code, scale = (step, width), (1, width)
        chunks = 2 * PIECES - CROSSING
        scratch = [
            vmem(inputs.shape, bf16), vmem((tasks, tokens, width), bf16), vmem((2, step, width), f32),
            vmem((na, 2, *code), i16), vmem((na, 2, *scale), f32), vmem((na, 2, *code), i16), vmem((na, 2, *scale), f32),
            vmem((na, 2, *code), i16), vmem((na, 2, *scale), f32), vmem((na, 2, *code), i16), vmem((na, 2, *scale), f32),
            vmem((nb, *code), i16), vmem((nb, *scale), f32), vmem((nb, *code), i16), vmem((nb, *scale), f32),
            vmem((2 * nb, 2, *code), i16), vmem((2 * nb, 2, *scale), f32),
            vmem((2 * nb, 2, *code), i16), vmem((2 * nb, 2, *scale), f32),
            vmem((tasks, blocks, step, width), f32),
            vmem((1, 128), f32), vmem((4 * tasks, 1, 128), f32),
            dma((4,)), dma, dma((tasks,)), dma((tasks,)),
            dma((na, 2)), dma((na, 2)), dma((na, 2, 2)), dma((na, 2, 2)),
            dma((nb, 2)), dma((nb, 2)), dma((2 * nb, 2, 2)), dma((2 * nb, 2, 2)),
            dma((4 * tasks,)), dma((4 * tasks,)),
            dma((2, chunks)), dma((2, chunks)), dma((2, CROSSING)), dma((2, CROSSING)), dma((PIECES,)), dma((PIECES,)),
        ]
        smem = pl.BlockSpec(memory_space=pltpu.SMEM)
        whole = pl.BlockSpec(memory_space=pltpu.VMEM)
        hbm = pl.BlockSpec(memory_space=pltpu.HBM)
        return pl.pallas_call(
            functools.partial(kernel, tasks, ndp, blocks),
            out_shape=jax.ShapeDtypeStruct((inputs.shape[1], width), jnp.bfloat16),
            in_specs=[smem, smem, hbm, hbm],
            out_specs=whole,
            scratch_shapes=scratch,
            compiler_params=pltpu.CompilerParams(collective_id=0, has_side_effects=True,
                                                 vmem_limit_bytes=44 * 1024 * 1024),
        )(*[pltpu.with_memory_space_constraint(v, pltpu.HBM) for v in (task_order, conflict_flags, inputs, cot)])

    return jax.shard_map(
        on_device, mesh=mesh,
        in_specs=(P("dp", None), P("task", "dp", None), P(), P()),
        out_specs=P(None, "task"), check_vma=False,
    )
```

```python
import functools

import jax
import jax.numpy as jnp
from jax import lax
from jax.experimental import pallas as pl
from jax.experimental.pallas import tpu as pltpu
from jax.sharding import PartitionSpec as P

MESH = pl.DeviceIdType.MESH
TOP = 32767.0
LAG = 3
PARTS = 1
SHARE = 13
REACH = 5
PIECES = 16
CROSSING = 12


def coded(tile):
    high = jnp.maximum(jnp.max(jnp.abs(tile), axis=0, keepdims=True), 1e-30)
    code = jnp.round(tile * (TOP / high)).astype(jnp.int32).astype(jnp.int16)
    return code, high * (1.0 / TOP)


def decoded(code, scale):
    return code.astype(jnp.int32).astype(jnp.float32) * scale


def shares(tasks, blocks):
    total = tasks * blocks * SHARE // 32
    return [(j + 1) * total // tasks - j * total // tasks for j in range(tasks)]


def kernel(tasks, ndp, blocks, order_hbm, flags_hbm, x_hbm, c_hbm, out_ref,
           order_ref, flags_ref, x_ref, cots, acc, ysend_a, yscale_a, yrecv_a, yrscale_a, zsend_a, zscale_a, zrecv_a, zrscale_a,
           ysend_b, yscale_b, yrecv_b, yrscale_b, zsend_b, zscale_b, zrecv_b, zrscale_b,
           grads, gram_own, gram_all,
           o_sem, x_sem, c_sem, cs_sem, cr_sem,
           yas_sem, yar_sem, zas_sem, zar_sem, ybs_sem, ybr_sem, zbs_sem, zbr_sem,
           gs_sem, gr_sem, zgs_sem, zgr_sem, ygs_sem, ygr_sem, yhs_sem, yhr_sem):
    nz = ndp // 2
    pairs_of = tasks // 2
    me_t = lax.axis_index("task")
    me_d = lax.axis_index("dp")
    z = me_d // 2
    y = me_d % 2
    step = acc.shape[1]
    width = cots.shape[2]
    rows = step * blocks
    of_b = shares(tasks, blocks)
    of_a = [blocks - n for n in of_b]
    base_a, base_b = [[sum(of[:j]) for j in range(tasks)] for of in (of_a, of_b)]
    units_a, units_b = sum(of_a), sum(of_b)
    at_end = (z == 0) | (z == nz - 1)

    def dp_at(zi, yi):
        return zi * 2 + yi

    def mate(j, way):
        return lax.rem(me_t // 2 + way * (j // 2) + pairs_of, pairs_of) * 2 + lax.rem(me_t % 2 + j % 2, 2)

    def slot(u, base):
        return sum(jnp.where(u >= first, 1, 0) for first in base[1:])

    def pick(u, base, values):
        return values[0] + sum(jnp.where(u >= base[j], values[j] - values[j - 1], 0) for j in range(1, tasks))

    def place_a(u):
        return slot(u, base_a), u - pick(u, base_a, base_a)

    def place_b(u):
        return slot(u, base_b), u - pick(u, base_b, [base_b[j] - of_a[j] for j in range(tasks)])

    partner = (me_t, dp_at(z, 1 - y))

    def remote(src, dst, s, r, device):
        return pltpu.make_async_remote_copy(src_ref=src, dst_ref=dst, send_sem=s, recv_sem=r,
                                            device_id=device, device_id_type=MESH)

    c_copy = pltpu.make_async_copy(c_hbm.at[:, pl.ds(pl.multiple_of(me_t * width, width), width)], cots.at[0], c_sem)
    c_copy.start()
    x_copies = []
    for d in range(4):
        part = pl.ds(pl.multiple_of(dp_at(d % 2, 1 - y if d < 2 else y) * rows, rows), rows)
        x_copies.append(pltpu.make_async_copy(x_hbm.at[:, part], x_ref.at[:, part], x_sem.at[d]))
        x_copies[-1].start()

    def hop(end):
        return z if end else nz - 1 - z

    def ahead(end):
        return (me_t, dp_at(jnp.clip(z + (1 if end else -1), 0, nz - 1), y))

    o_copies = [pltpu.make_async_copy(order_hbm, order_ref, o_sem.at[0]),
                pltpu.make_async_copy(flags_hbm, flags_ref, o_sem.at[1])]
    for copy in o_copies:
        copy.start()

    barrier = pltpu.get_barrier_semaphore()
    pl.semaphore_signal(barrier, inc=1, device_id=partner, device_id_type=MESH)
    for k in range(1, tasks):
        pl.semaphore_signal(barrier, inc=1, device_id=(lax.rem(me_t + k, tasks), me_d), device_id_type=MESH)
    for end in (0, 1):
        @pl.when(hop(end) < nz - 1)
        def _():
            pl.semaphore_signal(barrier, inc=1, device_id=ahead(end), device_id_type=MESH)
    pl.semaphore_wait(barrier, tasks + jnp.where(z > 0, 1, 0) + jnp.where(z < nz - 1, 1, 0))

    def c_remote(j):
        peer = mate(j, 1)
        return remote(c_hbm.at[:, pl.ds(pl.multiple_of(peer * width, width), width)], cots.at[j],
                      cs_sem.at[j], cr_sem.at[j], (peer, me_d))

    for j in range(1, tasks):
        c_remote(j).start()
    c_copy.wait()
    for copy in x_copies[:2]:
        copy.wait()

    def product(j, block, end, yi):
        first = pl.multiple_of((dp_at(end, yi) * blocks + block) * step, step)
        return lax.dot_general(x_ref[:, pl.ds(first, step)], cots[j], (((0,), (0,)), ((), ())),
                               preferred_element_type=jnp.float32)

    def ya(u):
        return (remote(ysend_a.at[u], yrecv_a.at[u], yas_sem.at[u, 0], yar_sem.at[u, 0], partner),
                remote(yscale_a.at[u], yrscale_a.at[u], yas_sem.at[u, 1], yar_sem.at[u, 1], partner))

    def yb(u):
        return (remote(ysend_b.at[u], yrecv_b.at[u], ybs_sem.at[u, 0], ybr_sem.at[u, 0], partner),
                remote(yscale_b.at[u], yrscale_b.at[u], ybs_sem.at[u, 1], ybr_sem.at[u, 1], partner))

    def za(u, end, h):
        device, at = ahead(end), (u, end, h)
        return (remote(zsend_a.at[at], zrecv_a.at[at], zas_sem.at[(*at, 0)], zar_sem.at[(*at, 0)], device),
                remote(zscale_a.at[at], zrscale_a.at[at], zas_sem.at[(*at, 1)], zar_sem.at[(*at, 1)], device))

    def zb(i, end):
        device = ahead(end)
        return (remote(zsend_b.at[i, end], zrecv_b.at[i, end], zbs_sem.at[i, end, 0], zbr_sem.at[i, end, 0], device),
                remote(zscale_b.at[i, end], zrscale_b.at[i, end], zbs_sem.at[i, end, 1], zbr_sem.at[i, end, 1], device))

    def start(copies):
        for copy in copies:
            copy.start()

    def arrive(copies):
        for copy in copies:
            copy.wait_recv()

    def each(first, last, body):
        if last > first:
            lax.fori_loop(first, last, lambda i, carry: (body(i), carry)[1], 0)

    def a_y(j, i):
        u = base_a[j] + i
        for end in (0, 1):
            code, scale = coded(product(j, i, end, 1 - y))
            ysend_a[u, end] = code
            yscale_a[u, end] = scale
        start(ya(u))

    def b_z(i, end):
        u, p = i // 2, i % 2
        j, block = place_b(u)
        acc[end] = product(j, block, end, lax.rem(1 - y + p, 2))

        @pl.when(hop(end) > 0)
        def _():
            arrive(zb(i, end))
            acc[end] = acc[end] + decoded(zrecv_b[i, end], zrscale_b[i, end])

        @pl.when(hop(end) < nz - 1)
        def _():
            code, scale = coded(acc[end])
            zsend_b[i, end] = code
            zscale_b[i, end] = scale
            start(zb(i, end))

        @pl.when((hop(end) == nz - 1) & (p == 0))
        def _():
            code, scale = coded(acc[end])
            ysend_b[u] = code
            yscale_b[u] = scale

            @pl.when(i >= held)
            def _():
                start(yb(u))

        @pl.when((hop(end) == nz - 1) & (p == 1))
        def _():
            grads[mate(j, -1), block] = acc[end]

    def a_z(u, end):
        j, block = place_a(u)
        acc[end] = product(j, block, end, y)

        @pl.when(hop(end) < hop(1 - end))
        def _():
            arrive(ya(u))
        acc[end] = acc[end] + decoded(yrecv_a[u, end], yrscale_a[u, end])

        for h in range(PARTS):
            part = pl.ds(h * (step // PARTS), step // PARTS)

            @pl.when(hop(end) > 0)
            def _():
                arrive(za(u, end, h))
                acc[end, part] = acc[end, part] + decoded(zrecv_a[u, end, h], zrscale_a[u, end, h])

            @pl.when(hop(end) < nz - 1)
            def _():
                code, scale = coded(acc[end, part])
                zsend_a[u, end, h] = code
                zscale_a[u, end, h] = scale
                start(za(u, end, h))

        @pl.when(hop(end) == nz - 1)
        def _():
            grads[mate(j, -1), block] = acc[end]

    def finish_b(u):
        j, block = place_b(u)
        arrive(yb(u))
        task = mate(j, -1)
        grads[task, block] = grads[task, block] + decoded(yrecv_b[u], yrscale_b[u])

    items_b = 2 * units_b
    held = max(items_b - LAG * (nz - 1), 0)

    def advance(s):
        for end in (1, 0):
            at = s - LAG * hop(end)

            @pl.when((at >= 0) & (at < items_b))
            def _():
                b_z(at, end)

            @pl.when((at >= items_b) & (at < items_b + units_a))
            def _():
                a_z(at - items_b, end)

    s = 0
    for j in range(tasks):
        if j:
            c_remote(j).wait_recv()
        steps = 2 * of_b[j]
        count = of_a[j]
        several = -(-count // steps)

        def both(i, first=s, j=j, count=count, several=several):
            for q in range(several):
                @pl.when((i - first) * several + q < count)
                def _():
                    a_y(j, (i - first) * several + q)
            advance(i)
        if j:
            each(s, s + steps, both)
        else:
            both(0)
            for copy in x_copies[2:]:
                copy.wait()
            each(1, steps, both)
        s += steps
    pl.when(at_end)(lambda: each(0, -(-held // 2), lambda u: start(yb(u))))
    total = items_b + units_a + LAG * (nz - 1)

    def last(i):
        advance(i)

        @pl.when(at_end & (i >= total - units_b))
        def _():
            finish_b(i - (total - units_b))
    each(s, total, last)

    for copy in o_copies:
        copy.wait()

    end_of = z // max(nz - 1, 1)
    mine = dp_at(end_of, y) * rows

    size = rows // PIECES
    chunks = 2 * PIECES - CROSSING

    def segment(end, yi, chunk):
        return out_ref.at[pl.ds(pl.multiple_of(dp_at(end, yi) * rows + chunk * size, size), size), :]

    def early(i):
        ref = segment(end_of, y, i)
        return remote(ref, ref, yhs_sem.at[i], yhr_sem.at[i], partner)

    def settle():
        def sent(copies):
            for copy in copies:
                copy.wait_send()

        for j in range(1, tasks):
            c_remote(j).wait_send()
        each(0, units_a, lambda u: sent(ya(u)))
        for end in (0, 1):
            @pl.when(hop(end) < nz - 1)
            def _():
                each(0, units_a, lambda u: [sent(za(u, end, h)) for h in range(PARTS)] and None)
                each(0, items_b, lambda i: sent(zb(i, end)))

    pl.when(jnp.logical_not(at_end))(settle)

    def weigh():
        pairs = [(s, t) for s in range(tasks) for t in range(s, tasks)]

        def products(index, sums):
            held = [grads[t, index] for t in range(tasks)]
            return tuple(total + jnp.sum((held[s] * held[t]).reshape(step // 8, 8, width), axis=0)
                         for total, (s, t) in zip(sums, pairs))

        sums = lax.fori_loop(0, blocks, products, tuple(jnp.zeros((8, width), jnp.float32) for _ in pairs))
        line = lax.broadcasted_iota(jnp.int32, (8, 128), 0)
        lane = lax.broadcasted_iota(jnp.int32, (8, 128), 1)
        spot = lane[:1]
        row = jnp.zeros((1, 128), jnp.float32)
        for place, total in enumerate(sums):
            value = jnp.sum(jnp.sum(total, axis=0, keepdims=True), axis=1, keepdims=True)
            row = row + jnp.where(spot == place, value, 0.0)

        def peer(k):
            end = k // 2 % 2
            return (lax.rem(me_t + k // 4, tasks), dp_at(nz - 1 - z if end else z, 1 - y if k % 2 else y))

        gram_own[...] = row
        copies = [remote(gram_own, gram_all.at[k], gs_sem.at[k], gr_sem.at[k], peer(k)) for k in range(1, 4 * tasks)]
        start(copies)
        settle()
        for u in range(units_b):
            for copy in yb(u):
                copy.wait_send()
        for k, copy in enumerate(copies, 1):
            copy.wait_recv()
            row = row + gram_all[k]

        gram = jnp.zeros((8, 128), jnp.float32)
        for place, (s, t) in enumerate(pairs):
            value = jnp.sum(jnp.where(spot == place, row, 0.0), axis=1, keepdims=True)
            here = ((line == s) & (lane == t)) | ((line == t) & (lane == s))
            gram = gram + jnp.where(here, value, 0.0)
        cols = [jnp.sum(jnp.where(lane == m, gram, 0.0), axis=1, keepdims=True) for m in range(tasks)]
        entry = lambda column, i: jnp.sum(jnp.where(line[:, :1] == i, column, 0.0), axis=0, keepdims=True)
        rank = line[:, :1]
        coefficients = [(rank == m).astype(jnp.float32) for m in range(tasks)]
        flag_cols = []
        for m in range(tasks):
            column = jnp.zeros((8, 1), jnp.float32)
            for i in range(tasks):
                column = column + jnp.where(rank == i, flags_ref[i, m].astype(jnp.float32), 0.0)
            flag_cols.append(column)
        for position in range(tasks):
            target = order_ref[position]
            picks = [jnp.where(target == m, 1.0, 0.0) for m in range(tasks)]
            column = sum(cols[m] * picks[m] for m in range(tasks))
            dots = sum(coefficients[m] * entry(column, m) for m in range(tasks))
            square = sum(entry(column, m) * picks[m] for m in range(tasks))
            active = sum(flag_cols[m] * picks[m] for m in range(tasks)) * jnp.where(rank == target, 0.0, 1.0)
            removed = jnp.minimum(dots, 0.0) / square * active
            coefficients = [coefficients[m] - removed * picks[m] for m in range(tasks)]
        weights = [jnp.sum(coefficients[m], axis=0, keepdims=True) for m in range(tasks)]

        def mix(index):
            mixed = sum(weights[t] * grads[t, index] for t in range(tasks))
            out_ref[pl.ds(pl.multiple_of(mine + index * step, step), step), :] = mixed.astype(jnp.bfloat16)

        first = CROSSING * blocks // PIECES
        each(first, blocks, mix)
        each(CROSSING, PIECES, lambda i: early(i).start())
        each(0, first, mix)
        for copy in copies:
            copy.wait_send()

    pl.when(at_end)(weigh)

    def along(end, i):
        chunk = jnp.where(i < PIECES, i, i - PIECES + CROSSING)
        ref = segment(end, jnp.where(i < PIECES, y, 1 - y), chunk)
        return remote(ref, ref, zgs_sem.at[end, i], zgr_sem.at[end, i], ahead(1 - end))

    def over(end, i):
        ref = segment(end, y, i)
        return remote(ref, ref, ygs_sem.at[end, i], ygr_sem.at[end, i], partner)

    def spread(s):
        for end in (0, 1):
            far = hop(1 - end)
            i = s - REACH * far

            @pl.when((i >= 0) & (i < chunks))
            def _():
                @pl.when(far > 0)
                def _():
                    along(end, i).wait_recv()

                @pl.when((far == 0) & (i >= PIECES))
                def _():
                    early(i - PIECES + CROSSING).wait_recv()

                @pl.when(far < nz - 1)
                def _():
                    along(end, i).start()

                @pl.when(i < CROSSING)
                def _():
                    over(end, i).start()

    each(0, chunks + REACH * (nz - 1), spread)

    def close(i):
        for end in (0, 1):
            over(end, i).wait_recv()
            over(end, i).wait_send()
    each(0, CROSSING, close)

    @pl.when(at_end)
    def _():
        each(CROSSING, PIECES, lambda i: early(i).wait_send())

    for end in (0, 1):
        @pl.when(hop(end) < nz - 1)
        def _():
            each(0, chunks, lambda i: along(1 - end, i).wait_send())


def solution(mesh):
    tasks, ndp = mesh.shape["task"], mesh.shape["dp"]

    def on_device(inputs, cotangent, task_order, conflict_flags):
        cot = cotangent[0]
        tokens = cot.shape[0]
        rows = inputs.shape[1] // 4
        step = min(rows, 128)
        blocks = rows // step
        width = cot.shape[1] // tasks
        nb = sum(shares(tasks, blocks))
        na = tasks * blocks - nb
        vmem, dma = pltpu.VMEM, pltpu.SemaphoreType.DMA
        f32, i16, bf16 = jnp.float32, jnp.int16, jnp.bfloat16
        code, scale = (step, width), (1, width)
        chunks = 2 * PIECES - CROSSING
        scratch = [
            pltpu.SMEM((tasks,), jnp.int32), pltpu.SMEM((tasks, tasks), jnp.int32),
            vmem(inputs.shape, bf16), vmem((tasks, tokens, width), bf16), vmem((2, step, width), f32),
            vmem((na, 2, *code), i16), vmem((na, 2, *scale), f32), vmem((na, 2, *code), i16), vmem((na, 2, *scale), f32),
            vmem((na, 2, PARTS, step // PARTS, width), i16), vmem((na, 2, PARTS, *scale), f32),
            vmem((na, 2, PARTS, step // PARTS, width), i16), vmem((na, 2, PARTS, *scale), f32),
            vmem((nb, *code), i16), vmem((nb, *scale), f32), vmem((nb, *code), i16), vmem((nb, *scale), f32),
            vmem((2 * nb, 2, *code), i16), vmem((2 * nb, 2, *scale), f32),
            vmem((2 * nb, 2, *code), i16), vmem((2 * nb, 2, *scale), f32),
            vmem((tasks, blocks, step, width), f32),
            vmem((1, 128), f32), vmem((4 * tasks, 1, 128), f32),
            dma((2,)), dma((4,)), dma, dma((tasks,)), dma((tasks,)),
            dma((na, 2)), dma((na, 2)), dma((na, 2, PARTS, 2)), dma((na, 2, PARTS, 2)),
            dma((nb, 2)), dma((nb, 2)), dma((2 * nb, 2, 2)), dma((2 * nb, 2, 2)),
            dma((4 * tasks,)), dma((4 * tasks,)),
            dma((2, chunks)), dma((2, chunks)), dma((2, CROSSING)), dma((2, CROSSING)), dma((PIECES,)), dma((PIECES,)),
        ]
        whole = pl.BlockSpec(memory_space=pltpu.VMEM)
        hbm = pl.BlockSpec(memory_space=pltpu.HBM)
        return pl.pallas_call(
            functools.partial(kernel, tasks, ndp, blocks),
            out_shape=jax.ShapeDtypeStruct((inputs.shape[1], width), jnp.bfloat16),
            in_specs=[hbm] * 4,
            out_specs=whole,
            scratch_shapes=scratch,
            compiler_params=pltpu.CompilerParams(collective_id=0, has_side_effects=True,
                                                 vmem_limit_bytes=44 * 1024 * 1024),
        )(*[pltpu.with_memory_space_constraint(v, pltpu.HBM) for v in (task_order, conflict_flags, inputs, cot)])

    return jax.shard_map(
        on_device, mesh=mesh,
        in_specs=(P("dp", None), P("task", "dp", None), P(), P()),
        out_specs=P(None, "task"), check_vma=False,
    )
```

```python
import functools

import jax
import jax.numpy as jnp
from jax import lax
from jax.experimental import pallas as pl
from jax.experimental.pallas import tpu as pltpu
from jax.sharding import PartitionSpec as P

MESH = pl.DeviceIdType.MESH
TOP = 32767.0
LAG = 3
PARTS = 1
SHARE = 13
REACH = 5
PIECES = 16
CROSSING = 12


def coded(tile):
    high = jnp.maximum(jnp.max(jnp.abs(tile), axis=0, keepdims=True), 1e-30)
    code = jnp.round(tile * (TOP / high)).astype(jnp.int32).astype(jnp.int16)
    return code, high * (1.0 / TOP)


def decoded(code, scale):
    return code.astype(jnp.int32).astype(jnp.float32) * scale


def shares(tasks, blocks):
    total = tasks * blocks * SHARE // 32
    return [(j + 1) * total // tasks - j * total // tasks for j in range(tasks)]


def kernel(tasks, ndp, blocks, order_hbm, flags_hbm, x_hbm, c_hbm, out_ref,
           order_ref, flags_ref, x_ref, cots, acc, ysend_a, yscale_a, yrecv_a, yrscale_a, zsend_a, zscale_a, zrecv_a, zrscale_a,
           ysend_b, yscale_b, yrecv_b, yrscale_b, zsend_b, zscale_b, zrecv_b, zrscale_b,
           grads, gram_own, gram_all,
           o_sem, x_sem, c_sem, cs_sem, cr_sem,
           yas_sem, yar_sem, zas_sem, zar_sem, ybs_sem, ybr_sem, zbs_sem, zbr_sem,
           gs_sem, gr_sem, zgs_sem, zgr_sem, ygs_sem, ygr_sem, yhs_sem, yhr_sem):
    nz = ndp // 2
    pairs_of = tasks // 2
    me_t = lax.axis_index("task")
    me_d = lax.axis_index("dp")
    z = me_d // 2
    y = me_d % 2
    step = acc.shape[1]
    width = cots.shape[2]
    rows = step * blocks
    of_b = shares(tasks, blocks)
    of_a = [blocks - n for n in of_b]
    base_a, base_b = [[sum(of[:j]) for j in range(tasks)] for of in (of_a, of_b)]
    units_a, units_b = sum(of_a), sum(of_b)
    at_end = (z == 0) | (z == nz - 1)

    def dp_at(zi, yi):
        return zi * 2 + yi

    def mate(j, way):
        return lax.rem(me_t // 2 + way * (j // 2) + pairs_of, pairs_of) * 2 + lax.rem(me_t % 2 + j % 2, 2)

    def slot(u, base):
        return sum(jnp.where(u >= first, 1, 0) for first in base[1:])

    def pick(u, base, values):
        return values[0] + sum(jnp.where(u >= base[j], values[j] - values[j - 1], 0) for j in range(1, tasks))

    def place_a(u):
        return slot(u, base_a), u - pick(u, base_a, base_a)

    def place_b(u):
        return slot(u, base_b), u - pick(u, base_b, [base_b[j] - of_a[j] for j in range(tasks)])

    partner = (me_t, dp_at(z, 1 - y))

    def remote(src, dst, s, r, device):
        return pltpu.make_async_remote_copy(src_ref=src, dst_ref=dst, send_sem=s, recv_sem=r,
                                            device_id=device, device_id_type=MESH)

    c_copy = pltpu.make_async_copy(c_hbm.at[:, pl.ds(pl.multiple_of(me_t * width, width), width)], cots.at[0], c_sem)
    c_copy.start()
    x_copies = []
    for d in range(4):
        part = pl.ds(pl.multiple_of(dp_at(d % 2, 1 - y if d < 2 else y) * rows, rows), rows)
        x_copies.append(pltpu.make_async_copy(x_hbm.at[:, part], x_ref.at[:, part], x_sem.at[d]))
        x_copies[-1].start()

    def hop(end):
        return z if end else nz - 1 - z

    def ahead(end):
        return (me_t, dp_at(jnp.clip(z + (1 if end else -1), 0, nz - 1), y))

    o_copies = [pltpu.make_async_copy(order_hbm, order_ref, o_sem.at[0]),
                pltpu.make_async_copy(flags_hbm, flags_ref, o_sem.at[1])]
    for copy in o_copies:
        copy.start()

    barrier = pltpu.get_barrier_semaphore()
    pl.semaphore_signal(barrier, inc=1, device_id=partner, device_id_type=MESH)
    for k in range(1, tasks):
        pl.semaphore_signal(barrier, inc=1, device_id=(lax.rem(me_t + k, tasks), me_d), device_id_type=MESH)
    for end in (0, 1):
        @pl.when(hop(end) < nz - 1)
        def _():
            pl.semaphore_signal(barrier, inc=1, device_id=ahead(end), device_id_type=MESH)
    pl.semaphore_wait(barrier, tasks + jnp.where(z > 0, 1, 0) + jnp.where(z < nz - 1, 1, 0))

    def c_remote(j):
        peer = mate(j, 1)
        return remote(c_hbm.at[:, pl.ds(pl.multiple_of(peer * width, width), width)], cots.at[j],
                      cs_sem.at[j], cr_sem.at[j], (peer, me_d))

    for j in range(1, tasks):
        c_remote(j).start()
    c_copy.wait()
    for copy in x_copies[:2]:
        copy.wait()

    def product(j, block, end, yi):
        first = pl.multiple_of((dp_at(end, yi) * blocks + block) * step, step)
        return lax.dot_general(x_ref[:, pl.ds(first, step)], cots[j], (((0,), (0,)), ((), ())),
                               preferred_element_type=jnp.float32)

    def ya(u):
        return (remote(ysend_a.at[u], yrecv_a.at[u], yas_sem.at[u, 0], yar_sem.at[u, 0], partner),
                remote(yscale_a.at[u], yrscale_a.at[u], yas_sem.at[u, 1], yar_sem.at[u, 1], partner))

    def yb(u):
        return (remote(ysend_b.at[u], yrecv_b.at[u], ybs_sem.at[u, 0], ybr_sem.at[u, 0], partner),
                remote(yscale_b.at[u], yrscale_b.at[u], ybs_sem.at[u, 1], ybr_sem.at[u, 1], partner))

    def za(u, end, h):
        device, at = ahead(end), (u, end, h)
        return (remote(zsend_a.at[at], zrecv_a.at[at], zas_sem.at[(*at, 0)], zar_sem.at[(*at, 0)], device),
                remote(zscale_a.at[at], zrscale_a.at[at], zas_sem.at[(*at, 1)], zar_sem.at[(*at, 1)], device))

    def zb(i, end):
        device = ahead(end)
        return (remote(zsend_b.at[i, end], zrecv_b.at[i, end], zbs_sem.at[i, end, 0], zbr_sem.at[i, end, 0], device),
                remote(zscale_b.at[i, end], zrscale_b.at[i, end], zbs_sem.at[i, end, 1], zbr_sem.at[i, end, 1], device))

    def start(copies):
        for copy in reversed(copies):
            copy.start()

    def arrive(copies):
        for copy in copies:
            copy.wait_recv()

    def each(first, last, body):
        if last > first:
            lax.fori_loop(first, last, lambda i, carry: (body(i), carry)[1], 0)

    def a_y(j, i):
        u = base_a[j] + i
        for end in (0, 1):
            code, scale = coded(product(j, i, end, 1 - y))
            yscale_a[u, end] = scale
            ysend_a[u, end] = code
        start(ya(u))

    def b_z(i, end):
        u, p = i // 2, i % 2
        j, block = place_b(u)
        acc[end] = product(j, block, end, lax.rem(1 - y + p, 2))

        @pl.when(hop(end) > 0)
        def _():
            arrive(zb(i, end))
            acc[end] = acc[end] + decoded(zrecv_b[i, end], zrscale_b[i, end])

        @pl.when(hop(end) < nz - 1)
        def _():
            code, scale = coded(acc[end])
            zscale_b[i, end] = scale
            zsend_b[i, end] = code
            start(zb(i, end))

        @pl.when((hop(end) == nz - 1) & (p == 0))
        def _():
            code, scale = coded(acc[end])
            yscale_b[u] = scale
            ysend_b[u] = code

            @pl.when(i >= held)
            def _():
                start(yb(u))

        @pl.when((hop(end) == nz - 1) & (p == 1))
        def _():
            grads[mate(j, -1), block] = acc[end]

    def a_z(u, end):
        j, block = place_a(u)
        acc[end] = product(j, block, end, y)

        @pl.when(hop(end) < hop(1 - end))
        def _():
            arrive(ya(u))
        acc[end] = acc[end] + decoded(yrecv_a[u, end], yrscale_a[u, end])

        for h in range(PARTS):
            part = pl.ds(h * (step // PARTS), step // PARTS)

            @pl.when(hop(end) > 0)
            def _():
                arrive(za(u, end, h))
                acc[end, part] = acc[end, part] + decoded(zrecv_a[u, end, h], zrscale_a[u, end, h])

            @pl.when(hop(end) < nz - 1)
            def _():
                code, scale = coded(acc[end, part])
                zscale_a[u, end, h] = scale
                zsend_a[u, end, h] = code
                start(za(u, end, h))

        @pl.when(hop(end) == nz - 1)
        def _():
            grads[mate(j, -1), block] = acc[end]

    def finish_b(u):
        j, block = place_b(u)
        arrive(yb(u))
        task = mate(j, -1)
        grads[task, block] = grads[task, block] + decoded(yrecv_b[u], yrscale_b[u])

    items_b = 2 * units_b
    held = max(items_b - LAG * (nz - 1), 0)

    def advance(s):
        for end in (1, 0):
            at = s - LAG * hop(end)

            @pl.when((at >= 0) & (at < items_b))
            def _():
                b_z(at, end)

            @pl.when((at >= items_b) & (at < items_b + units_a))
            def _():
                a_z(at - items_b, end)

    s = 0
    for j in range(tasks):
        if j:
            c_remote(j).wait_recv()
        steps = 2 * of_b[j]
        count = of_a[j]
        several = -(-count // steps)

        def both(i, first=s, j=j, count=count, several=several):
            for q in range(several):
                @pl.when((i - first) * several + q < count)
                def _():
                    a_y(j, (i - first) * several + q)
            advance(i)
        if j:
            each(s, s + steps, both)
        else:
            both(0)
            for copy in x_copies[2:]:
                copy.wait()
            each(1, steps, both)
        s += steps
    pl.when(at_end)(lambda: each(0, -(-held // 2), lambda u: start(yb(u))))
    total = items_b + units_a + LAG * (nz - 1)

    def last(i):
        advance(i)

        @pl.when(at_end & (i >= total - units_b))
        def _():
            finish_b(i - (total - units_b))
    each(s, total, last)

    for copy in o_copies:
        copy.wait()

    end_of = z // max(nz - 1, 1)
    mine = dp_at(end_of, y) * rows

    size = rows // PIECES
    chunks = 2 * PIECES - CROSSING

    def segment(end, yi, chunk):
        return out_ref.at[pl.ds(pl.multiple_of(dp_at(end, yi) * rows + chunk * size, size), size), :]

    def early(i):
        ref = segment(end_of, y, i)
        return remote(ref, ref, yhs_sem.at[i], yhr_sem.at[i], partner)

    def settle():
        def sent(copies):
            for copy in copies:
                copy.wait_send()

        for j in range(1, tasks):
            c_remote(j).wait_send()
        each(0, units_a, lambda u: sent(ya(u)))
        for end in (0, 1):
            @pl.when(hop(end) < nz - 1)
            def _():
                each(0, units_a, lambda u: [sent(za(u, end, h)) for h in range(PARTS)] and None)
                each(0, items_b, lambda i: sent(zb(i, end)))

    pl.when(jnp.logical_not(at_end))(settle)

    def weigh():
        pairs = [(s, t) for s in range(tasks) for t in range(s, tasks)]

        def products(index, sums):
            held = [grads[t, index] for t in range(tasks)]
            return tuple(total + jnp.sum((held[s] * held[t]).reshape(step // 8, 8, width), axis=0)
                         for total, (s, t) in zip(sums, pairs))

        sums = lax.fori_loop(0, blocks, products, tuple(jnp.zeros((8, width), jnp.float32) for _ in pairs))
        line = lax.broadcasted_iota(jnp.int32, (8, 128), 0)
        lane = lax.broadcasted_iota(jnp.int32, (8, 128), 1)
        spot = lane[:1]
        row = jnp.zeros((1, 128), jnp.float32)
        for place, total in enumerate(sums):
            value = jnp.sum(jnp.sum(total, axis=0, keepdims=True), axis=1, keepdims=True)
            row = row + jnp.where(spot == place, value, 0.0)

        def peer(k):
            end = k // 2 % 2
            return (lax.rem(me_t + k // 4, tasks), dp_at(nz - 1 - z if end else z, 1 - y if k % 2 else y))

        gram_own[...] = row
        copies = [remote(gram_own, gram_all.at[k], gs_sem.at[k], gr_sem.at[k], peer(k)) for k in range(1, 4 * tasks)]
        start(copies)
        settle()
        for u in range(units_b):
            for copy in yb(u):
                copy.wait_send()
        for k, copy in enumerate(copies, 1):
            copy.wait_recv()
            row = row + gram_all[k]

        gram = jnp.zeros((8, 128), jnp.float32)
        for place, (s, t) in enumerate(pairs):
            value = jnp.sum(jnp.where(spot == place, row, 0.0), axis=1, keepdims=True)
            here = ((line == s) & (lane == t)) | ((line == t) & (lane == s))
            gram = gram + jnp.where(here, value, 0.0)
        cols = [jnp.sum(jnp.where(lane == m, gram, 0.0), axis=1, keepdims=True) for m in range(tasks)]
        entry = lambda column, i: jnp.sum(jnp.where(line[:, :1] == i, column, 0.0), axis=0, keepdims=True)
        rank = line[:, :1]
        coefficients = [(rank == m).astype(jnp.float32) for m in range(tasks)]
        flag_cols = []
        for m in range(tasks):
            column = jnp.zeros((8, 1), jnp.float32)
            for i in range(tasks):
                column = column + jnp.where(rank == i, flags_ref[i, m].astype(jnp.float32), 0.0)
            flag_cols.append(column)
        for position in range(tasks):
            target = order_ref[position]
            picks = [jnp.where(target == m, 1.0, 0.0) for m in range(tasks)]
            column = sum(cols[m] * picks[m] for m in range(tasks))
            dots = sum(coefficients[m] * entry(column, m) for m in range(tasks))
            square = sum(entry(column, m) * picks[m] for m in range(tasks))
            active = sum(flag_cols[m] * picks[m] for m in range(tasks)) * jnp.where(rank == target, 0.0, 1.0)
            removed = jnp.minimum(dots, 0.0) / square * active
            coefficients = [coefficients[m] - removed * picks[m] for m in range(tasks)]
        weights = [jnp.sum(coefficients[m], axis=0, keepdims=True) for m in range(tasks)]

        def mix(index):
            mixed = sum(weights[t] * grads[t, index] for t in range(tasks))
            out_ref[pl.ds(pl.multiple_of(mine + index * step, step), step), :] = mixed.astype(jnp.bfloat16)

        first = CROSSING * blocks // PIECES
        each(first, blocks, mix)
        each(CROSSING, PIECES, lambda i: early(i).start())
        each(0, first, mix)
        for copy in copies:
            copy.wait_send()

    pl.when(at_end)(weigh)

    def along(end, i):
        chunk = jnp.where(i < PIECES, i, i - PIECES + CROSSING)
        ref = segment(end, jnp.where(i < PIECES, y, 1 - y), chunk)
        return remote(ref, ref, zgs_sem.at[end, i], zgr_sem.at[end, i], ahead(1 - end))

    def over(end, i):
        ref = segment(end, y, i)
        return remote(ref, ref, ygs_sem.at[end, i], ygr_sem.at[end, i], partner)

    def spread(s):
        for end in (0, 1):
            far = hop(1 - end)
            i = s - REACH * far

            @pl.when((i >= 0) & (i < chunks))
            def _():
                @pl.when(far > 0)
                def _():
                    along(end, i).wait_recv()

                @pl.when((far == 0) & (i >= PIECES))
                def _():
                    early(i - PIECES + CROSSING).wait_recv()

                @pl.when(far < nz - 1)
                def _():
                    along(end, i).start()

                @pl.when(i < CROSSING)
                def _():
                    over(end, i).start()

    each(0, chunks + REACH * (nz - 1), spread)

    def close(i):
        for end in (0, 1):
            over(end, i).wait_recv()
            over(end, i).wait_send()
    each(0, CROSSING, close)

    @pl.when(at_end)
    def _():
        each(CROSSING, PIECES, lambda i: early(i).wait_send())

    for end in (0, 1):
        @pl.when(hop(end) < nz - 1)
        def _():
            each(0, chunks, lambda i: along(1 - end, i).wait_send())


def solution(mesh):
    tasks, ndp = mesh.shape["task"], mesh.shape["dp"]

    def on_device(inputs, cotangent, task_order, conflict_flags):
        cot = cotangent[0]
        tokens = cot.shape[0]
        rows = inputs.shape[1] // 4
        step = min(rows, 128)
        blocks = rows // step
        width = cot.shape[1] // tasks
        nb = sum(shares(tasks, blocks))
        na = tasks * blocks - nb
        vmem, dma = pltpu.VMEM, pltpu.SemaphoreType.DMA
        f32, i16, bf16 = jnp.float32, jnp.int16, jnp.bfloat16
        code, scale = (step, width), (1, width)
        chunks = 2 * PIECES - CROSSING
        scratch = [
            pltpu.SMEM((tasks,), jnp.int32), pltpu.SMEM((tasks, tasks), jnp.int32),
            vmem(inputs.shape, bf16), vmem((tasks, tokens, width), bf16), vmem((2, step, width), f32),
            vmem((na, 2, *code), i16), vmem((na, 2, *scale), f32), vmem((na, 2, *code), i16), vmem((na, 2, *scale), f32),
            vmem((na, 2, PARTS, step // PARTS, width), i16), vmem((na, 2, PARTS, *scale), f32),
            vmem((na, 2, PARTS, step // PARTS, width), i16), vmem((na, 2, PARTS, *scale), f32),
            vmem((nb, *code), i16), vmem((nb, *scale), f32), vmem((nb, *code), i16), vmem((nb, *scale), f32),
            vmem((2 * nb, 2, *code), i16), vmem((2 * nb, 2, *scale), f32),
            vmem((2 * nb, 2, *code), i16), vmem((2 * nb, 2, *scale), f32),
            vmem((tasks, blocks, step, width), f32),
            vmem((1, 128), f32), vmem((4 * tasks, 1, 128), f32),
            dma((2,)), dma((4,)), dma, dma((tasks,)), dma((tasks,)),
            dma((na, 2)), dma((na, 2)), dma((na, 2, PARTS, 2)), dma((na, 2, PARTS, 2)),
            dma((nb, 2)), dma((nb, 2)), dma((2 * nb, 2, 2)), dma((2 * nb, 2, 2)),
            dma((4 * tasks,)), dma((4 * tasks,)),
            dma((2, chunks)), dma((2, chunks)), dma((2, CROSSING)), dma((2, CROSSING)), dma((PIECES,)), dma((PIECES,)),
        ]
        whole = pl.BlockSpec(memory_space=pltpu.VMEM)
        hbm = pl.BlockSpec(memory_space=pltpu.HBM)
        return pl.pallas_call(
            functools.partial(kernel, tasks, ndp, blocks),
            out_shape=jax.ShapeDtypeStruct((inputs.shape[1], width), jnp.bfloat16),
            in_specs=[hbm] * 4,
            out_specs=whole,
            scratch_shapes=scratch,
            compiler_params=pltpu.CompilerParams(collective_id=0, has_side_effects=True,
                                                 vmem_limit_bytes=44 * 1024 * 1024),
        )(*[pltpu.with_memory_space_constraint(v, pltpu.HBM) for v in (task_order, conflict_flags, inputs, cot)])

    return jax.shard_map(
        on_device, mesh=mesh,
        in_specs=(P("dp", None), P("task", "dp", None), P(), P()),
        out_specs=P(None, "task"), check_vma=False,
    )
```
